32 devices in a mesh: grp: 2 (over x), leaf: 16 (over z, y, core).
Axes of the slice: x: 2, y: 2, z: 4, core: 2. Of those that a mesh axis runs over, the one named last changes fastest.
Arguments:
- points: float32 [8, 32768], P(None, ('grp', 'leaf')), may hold values from -6 to 6
- rhs: float32 [16, 32768], P(None, ('grp', 'leaf')), may hold values from -6 to 6
- basis: float32 [32768, 128], P(('grp', 'leaf')), may hold values from -0.1875 to 0.1875
- transfer: float32 [32, 128, 128], P(('grp', 'leaf')), may hold values from -0.5 to 0.5
- noise: float32 [32768], P(('grp', 'leaf')), may hold values from 0.5 to 2
- inv_scale: float32 [8], replicated, may hold values from 0.15 to 0.6
- links: int32 [32, 2], P(('grp', 'leaf')), may hold values from 0 to 1, as said below
- leaf_skel: int32 [32, 128], P(('grp', 'leaf')), may hold values from 0 to 1023, as said below
- group_skel: int32 [2, 128], P('grp'), may hold values from 0 to 2047, as said below
Outputs:
- solution: float32 [16, 32768], P(None, ('grp', 'leaf'))
- residual: float32 [16, 32768], P(None, ('grp', 'leaf'))
The draws below stay inside these ranges and needn't reach their ends.
Inputs may be any that keep to these rules, and one draw needn't show every extreme that they name: `links`: column 1 of box l equals column 0 of box l + 1; column 0 is 0 for the first box of each group of 16 and column 1 for the last. `leaf_skel`: the 128 indices of a box are distinct. `group_skel`: the 128 indices of a group are distinct.
All inputs are finite; a program needn't handle non-finite values.
Results may differ from the reference program's by a relative error of at most 0.0003.
Values sent between devices are 32-bit elements; how exact they have to be, the bound alone decides.
No kernel may reach another device: no remote copies, remote signals or barrier semaphores. Data moves between devices by JAX's collectives and lax.ppermute only.
A program may use at most 128 MiB of HBM per device.

```python
import math
import jax
import jax.numpy as jnp
from jax import lax

PTS = 1024
DIM = 8
RHS = 16
SKEL = 128
ITERS = 2
BOXES = 16
GROUPS = 2
LEAVES = 32
NPTS = 32768


def draw_links(key, part):
    raw = jax.random.randint(jax.random.fold_in(key, 11), (LEAVES,), 0, 2)
    place = jnp.arange(LEAVES, dtype=jnp.int32) % BOXES
    upper = jnp.where(place == BOXES - 1, 0, raw)
    lower = jnp.concatenate([jnp.zeros((1,), jnp.int32), upper[:-1]])
    lower = jnp.where(place == 0, 0, lower)
    return jnp.stack([lower, upper], axis=1).astype(jnp.int32)


def draw_leaf_skel(key, part):
    keys = jax.random.split(jax.random.fold_in(key, 23), LEAVES)
    picks = jax.vmap(lambda one: jax.random.permutation(one, PTS)[:SKEL])(keys)
    return picks.astype(jnp.int32)


def draw_group_skel(key, part):
    keys = jax.random.split(jax.random.fold_in(key, 37), GROUPS)
    picks = jax.vmap(lambda one: jax.random.permutation(one, BOXES * SKEL)[:SKEL])(keys)
    return picks.astype(jnp.int32)


def steps_of(own_key, dims, pieces, smallest, top_value):
    level = 1.0
    for dim, parts in pieces:
        steps = jax.random.uniform(jax.random.fold_in(jax.random.fold_in(own_key, 6), dim), (parts,), jnp.float32, smallest / len(pieces), top_value / len(pieces))
        level = level * jnp.repeat(jnp.exp(steps), dims[dim] // parts).reshape((-1,) + (1,) * (len(dims) - 1 - dim))
    return level


def centred(own_key, dims, deviation, bound, cuts=(), kind=jnp.bfloat16):
    entries = jax.random.normal(own_key, dims, jnp.float32) * deviation
    if len(cuts) > 0:
        entries = steps_of(own_key, dims, cuts, -0.22, 0.18) * entries
    return jnp.clip(entries, min=-bound, max=bound).astype(kind)


def setup_inputs(seed: int = 0) -> dict:
    arg_keys = jax.random.split(jax.random.key(seed), 10)
    return {
        "points": centred(arg_keys[0], (DIM, NPTS), 1.0, 6.0, ((1, 32),), jnp.float32),
        "rhs": centred(arg_keys[1], (RHS, NPTS), 1.0, 6.0, ((1, 32),), jnp.float32),
        "basis": centred(arg_keys[2], (NPTS, SKEL), PTS ** -0.5, 0.1875, ((0, 32),), jnp.float32),
        "transfer": centred(arg_keys[3], (LEAVES, SKEL, SKEL), SKEL ** -0.5, 0.5, ((0, 32),), jnp.float32),
        "noise": jnp.clip(jnp.exp(math.log(2.0) - 1.3862944 * jax.random.uniform(arg_keys[4], (NPTS,), jnp.float32) ** steps_of(arg_keys[4], (NPTS,), ((0, 32),), -0.2, 0.2)), 0.5, 2.0),
        "inv_scale": jnp.clip(jnp.exp(jax.random.uniform(arg_keys[5], (DIM,), jnp.float32, math.log(0.15), math.log(0.6))), 0.15, 0.6),
        "links": draw_links(jax.random.fold_in(arg_keys[9], 71), 0),
        "leaf_skel": draw_leaf_skel(jax.random.fold_in(arg_keys[9], 71), 0),
        "group_skel": draw_group_skel(jax.random.fold_in(arg_keys[9], 71), 0),
    }


def kernel_block(left, right, inv_scale):
    first = left * inv_scale[:, None]
    second = right * inv_scale[:, None]
    cross = lax.dot_general(first, second, (((0,), (0,)), ((), ())), precision=lax.Precision.HIGHEST)
    dist = lax.optimization_barrier(jnp.sum(first * first, axis=0))[:, None] + lax.optimization_barrier(jnp.sum(second * second, axis=0))[None, :] - 2.0 * cross
    scaled = jnp.sqrt(5.0 * jnp.maximum(dist, 0.0))
    return (1.0 + scaled + scaled * scaled / 3.0) * jnp.exp(-scaled)

def contract(first, second):
    return lax.dot_general(first, second, (((1,), (1,)), ((), ())), precision=lax.Precision.HIGHEST)

def product(first, second):
    return jnp.dot(first, second, precision=lax.Precision.HIGHEST)

def reference(points, rhs, basis, transfer, noise, inv_scale, links, leaf_skel, group_skel):
    leaf_pts = points.reshape(DIM, LEAVES, PTS).transpose(1, 0, 2)
    skel_pts = jnp.take_along_axis(leaf_pts, leaf_skel[:, None, :], axis=2)
    group_pts = skel_pts.reshape(GROUPS, BOXES, DIM, SKEL).transpose(0, 2, 1, 3).reshape(GROUPS, DIM, BOXES * SKEL)
    top_pts = jnp.take_along_axis(group_pts, group_skel[:, None, :], axis=2)
    top_all = top_pts.transpose(1, 0, 2).reshape(DIM, GROUPS * SKEL)
    leaf_basis = basis.reshape(LEAVES, PTS, SKEL)
    leaf_noise = noise.reshape(LEAVES, PTS)
    bits = links.astype(jnp.float32)

    def apply(vec):
        leaf_vec = vec.reshape(RHS, LEAVES, PTS).transpose(1, 0, 2)
        coeff = jnp.einsum('lrm,lms->lrs', leaf_vec, leaf_basis, precision=lax.Precision.HIGHEST)
        lifted = jnp.einsum('lrs,lst->lrt', coeff, transfer, precision=lax.Precision.HIGHEST)
        group_coeff = lifted.reshape(GROUPS, BOXES, RHS, SKEL).sum(axis=1)
        top_coeff = group_coeff.transpose(1, 0, 2).reshape(RHS, GROUPS * SKEL)
        box_coeff = coeff.reshape(GROUPS, BOXES, RHS, SKEL).transpose(0, 2, 1, 3).reshape(GROUPS, RHS, BOXES * SKEL)

        def one_leaf(index):
            group = index // BOXES
            lower = jnp.maximum(index - 1, 0)
            upper = jnp.minimum(index + 1, LEAVES - 1)
            own = leaf_pts[index]
            far = contract(box_coeff[group], kernel_block(skel_pts[index], group_pts[group], inv_scale))
            top = contract(top_coeff, kernel_block(top_pts[group], top_all, inv_scale))
            row = far + contract(top, transfer[index])
            total = contract(row, leaf_basis[index])
            left_bit = bits[index, 0]
            right_bit = bits[index, 1]
            near = (1.0 + left_bit + right_bit) * product(leaf_vec[index], kernel_block(own, own, inv_scale))
            near = near + left_bit * product(leaf_vec[lower], kernel_block(leaf_pts[lower], own, inv_scale))
            near = near + right_bit * product(leaf_vec[upper], kernel_block(leaf_pts[upper], own, inv_scale))
            return leaf_noise[index][None, :] * leaf_vec[index] + near + total
        result = lax.map(one_leaf, jnp.arange(LEAVES, dtype=jnp.int32))
        return result.transpose(1, 0, 2).reshape(RHS, NPTS)
    solution = jnp.zeros_like(rhs)
    residual = rhs
    direction = rhs
    norm_now = lax.optimization_barrier(jnp.sum(residual * residual, axis=1))
    for step in range(ITERS):
        image = apply(direction)
        alpha = norm_now / lax.optimization_barrier(jnp.sum(direction * image, axis=1))
        solution = solution + alpha[:, None] * direction
        residual = residual - alpha[:, None] * image
        if step + 1 < ITERS:
            norm_next = lax.optimization_barrier(jnp.sum(residual * residual, axis=1))
            direction = residual + (norm_next / norm_now)[:, None] * direction
            norm_now = norm_next
    return (solution, residual)
```

```python
import functools
import math

import jax
import jax.numpy as jnp
from jax import lax
from jax.experimental import pallas as pl
from jax.experimental.pallas import tpu as pltpu
from jax.sharding import PartitionSpec as P

HIGH = lax.Precision.HIGHEST
F32 = jnp.float32
BF16 = jnp.bfloat16
LOG2E = math.log2(math.e)
LN2 = math.log(2.0)
UNIT = math.sqrt(5.0) * LOG2E
MIB = 1 << 20


def dot(first, second, precision=HIGH):
    return lax.dot_general(
        first, second, (((1,), (0,)), ((), ())), precision=precision, preferred_element_type=F32
    )


def dot_t(first, second):
    return lax.dot_general(
        first, second, (((1,), (1,)), ((), ())), precision=HIGH, preferred_element_type=F32
    )


def raw(first, second):
    return dot(first, second, lax.Precision.DEFAULT)


def split3(value):
    high = value.astype(BF16).astype(F32)
    rest = value - high
    middle = rest.astype(BF16).astype(F32)
    return high, middle, (rest - middle).astype(BF16).astype(F32)


def norm_rows(scaled):
    high, middle, low = split3(jnp.sum(scaled * scaled, axis=0, keepdims=True))
    one = jnp.ones_like(high)
    zero = jnp.zeros((2,) + high.shape[1:], F32)
    return high, middle, low, one, zero


def stack_left(scaled):
    high, middle, low = split3(scaled)
    n_high, n_middle, n_low, one, zero = norm_rows(scaled)
    norms = jnp.concatenate([n_high, n_middle, n_low, one, one, one, zero], axis=0)
    rows = [high, high, middle, middle, high, low, norms]
    used = 6 * scaled.shape[0] + 8
    rows.append(jnp.zeros((128 - used, scaled.shape[1]), F32))
    return jnp.concatenate(rows, axis=0).T.astype(BF16)


def stack_right(scaled):
    high, middle, low = split3(-2.0 * scaled)
    n_high, n_middle, n_low, one, zero = norm_rows(scaled)
    norms = jnp.concatenate([one, one, one, n_high, n_middle, n_low, zero], axis=0)
    rows = [high, middle, high, middle, low, high, norms]
    used = 6 * scaled.shape[0] + 8
    rows.append(jnp.zeros((128 - used, scaled.shape[1]), F32))
    return jnp.concatenate(rows, axis=0).astype(BF16)


def matern(square):
    square = jnp.maximum(square, 1e-30)
    root = square * lax.rsqrt(square)
    return (1.0 + root * (LN2 + (LN2 * LN2 / 3.0) * root)) * jnp.exp2(-root)


def diagonal_mask(rows):
    shape = (rows, 128)
    return lax.broadcasted_iota(jnp.int32, shape, 0) == lax.broadcasted_iota(jnp.int32, shape, 1)


def to_row(column):
    rows = column.shape[0]
    return jnp.sum(jnp.where(diagonal_mask(rows), column, 0.0), axis=0, keepdims=True)


def to_column(row, rows, start=0):
    shape = (rows, 128)
    lane = lax.broadcasted_iota(jnp.int32, shape, 1)
    mask = lane == lax.broadcasted_iota(jnp.int32, shape, 0) + start
    return jnp.sum(jnp.where(mask, row, 0.0), axis=1, keepdims=True)


def row_sum(value):
    return jnp.sum(value, axis=1, keepdims=True)


def each(count, body, init):
    if count <= 16:
        for index in range(count):
            init = body(index, init)
        return init
    return lax.fori_loop(0, count, body, init)


def call(kernel, outs, ins, smem=(), scratch=(), limit=8, flops=1_000_000, name=None):
    space = [pltpu.SMEM if i in smem else pltpu.VMEM for i in range(len(ins))]
    return pl.pallas_call(
        kernel,
        out_shape=[jax.ShapeDtypeStruct(s, d) for s, d in outs],
        in_specs=[pl.BlockSpec(memory_space=s) for s in space],
        out_specs=[pl.BlockSpec(memory_space=pltpu.VMEM) for _ in outs],
        scratch_shapes=list(scratch),
        compiler_params=pltpu.CompilerParams(vmem_limit_bytes=limit * MIB),
        cost_estimate=pl.CostEstimate(flops=flops, bytes_accessed=1 << 20, transcendentals=0),
        name=name,
    )(*ins)


def prepare_kernel(
    points_ref, rhs_ref, basis_ref, lift_ref, noise_ref, scale_ref, links_ref, skel_ref,
    beside_ref, send_ref,
):
    dim, width = points_ref.shape
    rhs_rows = rhs_ref.shape[0]
    boxes, rows, skel = send_ref.shape
    sub = lax.broadcasted_iota(jnp.int32, (dim, 1), 0)
    scale = jnp.zeros((dim, 1), F32)
    for d in range(dim):
        scale = jnp.where(sub == d, scale_ref[d], scale)
    scaled = points_ref[...] * scale * UNIT
    rhs = rhs_ref[...]
    beside_ref[0:dim, :] = scaled
    beside_ref[dim:, :] = rhs
    pick = lax.broadcasted_iota(jnp.int32, (width, skel), 0) == skel_ref[...]
    pick = jnp.where(pick, 1.0, 0.0).astype(BF16)
    parts = raw(jnp.concatenate(split3(scaled), axis=0).astype(BF16), pick)
    chosen = parts[0:dim] + parts[dim : 2 * dim] + parts[2 * dim :]
    coeff = dot(rhs, basis_ref[...])
    lifted = dot(coeff, lift_ref[0])
    weight = noise_ref[...] + (1 + links_ref[0, 0] + links_ref[0, 1]).astype(F32)
    square = rhs * rhs
    total = to_row(row_sum(square))
    weighted = to_row(row_sum(square * weight))
    rest = jnp.zeros((rows - dim - 2 * rhs_rows - 2, skel), F32)
    block = jnp.concatenate([chosen, coeff, lifted, total, weighted, rest], axis=0)

    def put(index, carry):
        send_ref[index] = block
        return carry

    each(boxes, put, 0)


def near_kernel(links_ref, own_ref, other_ref, high_ref, low_ref, out_ref, dist_ref, *, kind):
    rhs_rows, width = out_ref.shape
    dim = own_ref.shape[0] - rhs_rows
    block = dist_ref.shape[0]
    chunk = 32
    if kind < 0:
        weight = 1 + links_ref[0, 0] + links_ref[0, 1]
    else:
        parity = lax.rem(lax.axis_index("leaf"), 2)
        side = 1 - parity if kind == 0 else parity
        weight = links_ref[0, 0] * (1 - side) + links_ref[0, 1] * side

    @pl.when(weight > 0)
    def _():
        left = stack_left(other_ref[0:dim, :])
        right = stack_right(own_ref[0:dim, :])
        vec = jnp.concatenate(split3(other_ref[dim:, :]), axis=0).astype(BF16)
        total = jnp.zeros((3 * rhs_rows, width), F32)
        for i in range(width // block):
            rows = slice(i * block, (i + 1) * block)
            dist_ref[...] = raw(left[rows], right)
            for j in range(block // chunk):
                value = matern(dist_ref[j * chunk : (j + 1) * chunk, :])
                high = value.astype(BF16)
                at = slice(i * block + j * chunk, i * block + (j + 1) * chunk)
                high_ref[at, :] = high
                low_ref[at, :] = (value - high.astype(F32)).astype(BF16)
            total = total + raw(vec[:, rows], high_ref[rows, :])
            total = total + raw(vec[:, rows], low_ref[rows, :])
        result = total[0:rhs_rows] + total[rhs_rows : 2 * rhs_rows] + total[2 * rhs_rows :]
        out_ref[...] = result * weight.astype(F32)

    @pl.when(weight <= 0)
    def _():
        out_ref[...] = jnp.zeros_like(out_ref)


def near_again_kernel(links_ref, vec_ref, high_ref, low_ref, out_ref, *, kind):
    rhs_rows, width = out_ref.shape
    if kind < 0:
        weight = 1 + links_ref[0, 0] + links_ref[0, 1]
    else:
        parity = lax.rem(lax.axis_index("leaf"), 2)
        side = 1 - parity if kind == 0 else parity
        weight = links_ref[0, 0] * (1 - side) + links_ref[0, 1] * side

    @pl.when(weight > 0)
    def _():
        vec = jnp.concatenate(split3(vec_ref[...]), axis=0).astype(BF16)
        total = raw(vec, high_ref[...]) + raw(vec, low_ref[...])
        result = total[0:rhs_rows] + total[rhs_rows : 2 * rhs_rows] + total[2 * rhs_rows :]
        out_ref[...] = result * weight.astype(F32)

    @pl.when(weight <= 0)
    def _():
        out_ref[...] = jnp.zeros_like(out_ref)


def group_kernel(got_ref, pick_ref, out_ref, *, dim, rhs_rows):
    boxes, rows, skel = got_ref.shape
    start = dim + rhs_rows

    def body(index, carry):
        chosen, summed = carry
        block = got_ref[index]
        pick = lax.broadcasted_iota(jnp.int32, (skel, skel), 0) + index * skel == pick_ref[...]
        pick = jnp.where(pick, 1.0, 0.0).astype(BF16)
        parts = jnp.concatenate(split3(block[0:dim]), axis=0).astype(BF16)
        return chosen + raw(parts, pick), summed + block[start:]

    zero = (jnp.zeros((3 * dim, skel), F32), jnp.zeros((rows - start, skel), F32))
    chosen, summed = each(boxes, body, zero)
    out_ref[0:dim, :] = chosen[0:dim] + chosen[dim : 2 * dim] + chosen[2 * dim :]
    out_ref[dim:, :] = summed


def far_kernel(got_ref, mine_ref, matrix_ref, out_ref, *, dim):
    rhs_rows, skel = out_ref.shape
    right = stack_right(mine_ref[0, 0:dim, :])

    def body(index, total):
        block = got_ref[index]
        matrix = matern(raw(stack_left(block[0:dim]), right))
        matrix_ref[index] = matrix
        return total + dot(block[dim : dim + rhs_rows], matrix)

    out_ref[...] = each(got_ref.shape[0], body, jnp.zeros((rhs_rows, skel), F32))


def far_again_kernel(got_ref, matrix_ref, out_ref):
    rhs_rows, skel = out_ref.shape

    def body(index, total):
        return total + dot(got_ref[index, 0:rhs_rows, :], matrix_ref[index])

    out_ref[...] = each(got_ref.shape[0], body, jnp.zeros((rhs_rows, skel), F32))


def sum_kernel(got_ref, out_ref):
    start = got_ref.shape[1] - out_ref.shape[0]

    def body(index, total):
        return total + got_ref[index, start:, :]

    out_ref[...] = each(got_ref.shape[0], body, jnp.zeros(out_ref.shape, F32))


def first_image_kernel(
    *refs, dim, others,
):
    mine_ref = refs[0]
    other_refs = refs[1 : 1 + others]
    (far_ref, near_ref, near_a_ref, near_b_ref, rhs_ref, noise_ref, lift_ref, basis_ref,
     shift_ref, sigma_ref, send_ref, matrix_ref) = refs[1 + others :]
    rhs_rows = rhs_ref.shape[0]
    boxes, rows, skel = send_ref.shape
    right = stack_right(mine_ref[0:dim, :])
    top = jnp.zeros((rhs_rows, skel), F32)
    sums = jnp.zeros((8, skel), F32)
    for index, ref in enumerate((mine_ref,) + tuple(other_refs)):
        matrix = matern(raw(stack_left(ref[0:dim, :]), right))
        matrix_ref[index] = matrix
        top = top + dot(ref[dim : dim + rhs_rows, :], matrix)
        sums = sums + ref[dim + rhs_rows : dim + rhs_rows + 8, :]
    total = sums[0:1]
    lane = lax.broadcasted_iota(jnp.int32, (1, skel), 1)
    sigma = jnp.where(lane < rhs_rows, sums[1:2] / jnp.maximum(total, 1e-30), 0.0)
    sigma = to_column(sigma, rhs_rows)
    rhs = rhs_ref[...]
    row = far_ref[...] + dot_t(top, lift_ref[0])
    near = near_ref[...] + near_a_ref[...] + near_b_ref[...]
    shift = (noise_ref[...] - sigma) * rhs + near + dot_t(row, basis_ref[...])
    shift_ref[...] = shift
    sigma_ref[...] = jnp.broadcast_to(sigma, sigma_ref.shape)
    coeff = dot(shift, basis_ref[...])
    lifted = dot(coeff, lift_ref[0])
    curve = to_row(row_sum(rhs * shift))
    rest = jnp.zeros((rows - 2 * rhs_rows - 2, skel), F32)
    block = jnp.concatenate([coeff, lifted, total, curve, rest], axis=0)

    def put(index, carry):
        send_ref[index] = block
        return carry

    each(boxes, put, 0)


def second_image_kernel(
    *refs, others, boxes,
):
    mine_ref = refs[0]
    other_refs = refs[1 : 1 + others]
    (far_ref, near_ref, near_a_ref, near_b_ref, rhs_ref, shift_ref, sigma_ref, noise_ref,
     lift_ref, basis_ref, matrix_ref, residual_ref, image_ref, alpha_ref, send_ref) = refs[1 + others :]
    rhs_rows = rhs_ref.shape[0]
    skel = lift_ref.shape[2]
    top = jnp.zeros((rhs_rows, skel), F32)
    total = None
    sums = jnp.zeros((8, skel), F32)
    for index, ref in enumerate((mine_ref,) + tuple(other_refs)):
        top = top + dot(ref[0:rhs_rows, :], matrix_ref[index])
        sums = sums + ref[rhs_rows : rhs_rows + 8, :]
    total = to_column(mine_ref[rhs_rows : rhs_rows + 1, :], rhs_rows) * (1.0 / boxes)
    along = to_column(sums[1:2], rhs_rows)
    sigma = sigma_ref[:, 0:1]
    curve = along + sigma * total
    alpha = total / curve
    keep = along / curve
    shift = shift_ref[...]
    rhs = rhs_ref[...]
    row = far_ref[...] + dot_t(top, lift_ref[0])
    near = near_ref[...] + near_a_ref[...] + near_b_ref[...]
    second = noise_ref[...] * shift + near + dot_t(row, basis_ref[...])
    residual = keep * rhs - alpha * shift
    image = keep * (shift + sigma * rhs) - alpha * second
    residual_ref[...] = residual
    image_ref[...] = image
    alpha_ref[0:rhs_rows] = jnp.broadcast_to(alpha, (rhs_rows, skel))
    alpha_ref[rhs_rows:] = jnp.broadcast_to(total, (rhs_rows, skel))
    lane = lax.broadcasted_iota(jnp.int32, (rhs_rows, skel), 1)
    index = lax.broadcasted_iota(jnp.int32, (rhs_rows, skel), 0)
    both = jnp.where(lane == index, row_sum(residual * residual), 0.0)
    both = both + jnp.where(lane == index + rhs_rows, row_sum(residual * image), 0.0)
    both = jnp.sum(both, axis=0, keepdims=True)

    def put(index, carry):
        send_ref[index] = both
        return carry

    each(send_ref.shape[0], put, 0)


def finish_kernel(
    got_ref, alpha_ref, rhs_ref, shift_ref, sigma_ref, residual_ref, image_ref, solution_ref, out_ref
):
    rhs_rows = rhs_ref.shape[0]
    sums = jnp.sum(got_ref[...], axis=0)
    norm_next = to_column(sums, rhs_rows)
    curve = to_column(sums, rhs_rows, rhs_rows)
    alpha = alpha_ref[0:rhs_rows, 0:1]
    norm_now = alpha_ref[rhs_rows:, 0:1]
    ratio = norm_next / norm_now
    step = norm_next / (curve - ratio * norm_next / alpha)
    rhs = rhs_ref[...]
    residual = residual_ref[...]
    image = shift_ref[...] + sigma_ref[:, 0:1] * rhs
    solution_ref[...] = alpha * rhs + step * (residual + ratio * rhs)
    out_ref[...] = residual - step * (image_ref[...] + ratio * image)


def spread(value, axis):
    return lax.all_to_all(value, axis, 0, 0, tiled=True)


def local(points, rhs, basis, transfer, noise, inv_scale, links, leaf_skel, group_skel):
    dim, width = points.shape
    rhs_rows = rhs.shape[0]
    skel = basis.shape[1]
    boxes = lax.axis_size("leaf")
    groups = lax.axis_size("grp")
    noise = noise[None, :]
    pairs_a = [(i, i ^ 1) for i in range(boxes) if (i ^ 1) < boxes]
    pairs_b = [(i, ((i + 1) ^ 1) - 1) for i in range(boxes) if 0 <= ((i + 1) ^ 1) - 1 < boxes]
    wide = (rhs_rows, width)
    small = (rhs_rows, skel)
    near_flops = 4 * 10**9

    rows = -(-(dim + 2 * rhs_rows + 2) // 8) * 8
    beside, send = call(
        prepare_kernel,
        [((dim + rhs_rows, width), F32), ((boxes, rows, skel), F32)],
        [points, rhs, basis, transfer, noise, inv_scale, links, leaf_skel],
        smem=(5, 6), name="prepare",
    )
    beside_a = lax.ppermute(beside, "leaf", pairs_a)
    beside_b = lax.ppermute(beside, "leaf", pairs_b)
    got = spread(send, "leaf")

    def near_first(other, kind):
        return call(
            functools.partial(near_kernel, kind=kind),
            [((width, width), BF16), ((width, width), BF16), (wide, F32)],
            [links, beside, other],
            smem=(0,), scratch=[pltpu.VMEM((256, width), F32)], limit=16, flops=near_flops,
            name="near",
        )

    high, low, near = near_first(beside, -1)
    high_a, low_a, near_a = near_first(beside_a, 0)
    high_b, low_b, near_b = near_first(beside_b, 1)

    def exchange(value):
        return [
            lax.ppermute(value, "grp", [(i, (i + s) % groups) for i in range(groups)])
            for s in range(1, groups)
        ]

    (mine,) = call(
        functools.partial(group_kernel, dim=dim, rhs_rows=rhs_rows),
        [((rows - rhs_rows, skel), F32)], [got, group_skel], name="group",
    )
    others = exchange(mine)
    far_matrix, far = call(
        functools.partial(far_kernel, dim=dim),
        [((boxes, skel, skel), F32), (small, F32)], [got, send], limit=16, flops=10**9, name="far",
    )
    rows_next = -(-(2 * rhs_rows + 2) // 8) * 8
    shift, sigma, send, top_matrix = call(
        functools.partial(first_image_kernel, dim=dim, others=groups - 1),
        [(wide, F32), (small, F32), ((boxes, rows_next, skel), F32), ((groups, skel, skel), F32)],
        [mine, *others, far, near, near_a, near_b, rhs, noise, transfer, basis], name="image",
    )
    shift_a = lax.ppermute(shift, "leaf", pairs_a)
    shift_b = lax.ppermute(shift, "leaf", pairs_b)
    got = spread(send, "leaf")

    def near_next(vec, high, low, kind):
        return call(
            functools.partial(near_again_kernel, kind=kind),
            [(wide, F32)], [links, vec, high, low], smem=(0,), limit=16, flops=10**9, name="again",
        )[0]

    near = near_next(shift, high, low, -1)
    near_a = near_next(shift_a, high_a, low_a, 0)
    near_b = near_next(shift_b, high_b, low_b, 1)
    (mine,) = call(sum_kernel, [((rows_next - rhs_rows, skel), F32)], [got], name="sums")
    others = exchange(mine)
    (far,) = call(far_again_kernel, [(small, F32)], [got, far_matrix], flops=10**8, name="faragain")
    residual, image, alpha, send = call(
        functools.partial(second_image_kernel, others=groups - 1, boxes=boxes),
        [(wide, F32), (wide, F32), ((2 * rhs_rows, skel), F32), ((boxes * groups, 1, skel), F32)],
        [mine, *others, far, near, near_a, near_b, rhs, shift, sigma, noise, transfer, basis, top_matrix],
        name="second",
    )
    got = spread(send, ("grp", "leaf"))
    return tuple(
        call(
            finish_kernel, [(wide, F32), (wide, F32)],
            [got, alpha, rhs, shift, sigma, residual, image], name="finish",
        )
    )


def solution(mesh):
    return jax.shard_map(
        local,
        mesh=mesh,
        in_specs=(
            P(None, ("grp", "leaf")),
            P(None, ("grp", "leaf")),
            P(("grp", "leaf"), None),
            P(("grp", "leaf"), None, None),
            P(("grp", "leaf")),
            P(),
            P(("grp", "leaf"), None),
            P(("grp", "leaf"), None),
            P("grp", None),
        ),
        out_specs=(P(None, ("grp", "leaf")), P(None, ("grp", "leaf"))),
        check_vma=False,
    )
```

```python
import functools
import math

import jax
import jax.numpy as jnp
from jax import lax
from jax.experimental import pallas as pl
from jax.experimental.pallas import tpu as pltpu
from jax.sharding import PartitionSpec as P

F32 = jnp.float32
BF16 = jnp.bfloat16
LOG2E = math.log2(math.e)
UNIT = math.sqrt(5.0)
THIRD = 1.0 / 3.0
MIB = 1 << 20


def raw(first, second):
    return lax.dot_general(
        first, second, (((1,), (0,)), ((), ())), preferred_element_type=F32
    )


def raw_t(first, second):
    return lax.dot_general(
        first, second, (((1,), (1,)), ((), ())), preferred_element_type=F32
    )


def split3(value):
    high = value.astype(BF16).astype(F32)
    rest = value - high
    middle = rest.astype(BF16).astype(F32)
    return high, middle, (rest - middle).astype(BF16).astype(F32)


def split2(value):
    high = value.astype(BF16)
    return high, (value - high.astype(F32)).astype(BF16)


def triple(value):
    return jnp.concatenate(split3(value), axis=0).astype(BF16)


def fold(value):
    rows = value.shape[0] // 3
    return value[0:rows] + value[rows : 2 * rows] + value[2 * rows :]


def pair(value):
    return jnp.concatenate(split2(value), axis=1)


def times(first, second):
    half = second.shape[1] // 2
    both = fold(raw(triple(first), second))
    return both[:, :half] + both[:, half:]


def times_t(first, second):
    parts = triple(first)
    return fold(raw_t(jnp.concatenate([parts, parts], axis=1), second))


def times_parts_t(first, high, low):
    parts = triple(first)
    return fold(raw_t(parts, high) + raw_t(parts, low))


def norm_rows(scaled):
    high, middle, low = split3(jnp.sum(scaled * scaled, axis=0, keepdims=True))
    one = jnp.ones_like(high)
    zero = jnp.zeros((2,) + high.shape[1:], F32)
    return high, middle, low, one, zero


def stack_left(scaled):
    high, middle, low = split3(scaled)
    n_high, n_middle, n_low, one, zero = norm_rows(scaled)
    norms = jnp.concatenate([n_high, n_middle, n_low, one, one, one, zero], axis=0)
    rows = [high, high, middle, middle, high, low, norms]
    used = 6 * scaled.shape[0] + 8
    rows.append(jnp.zeros((128 - used, scaled.shape[1]), F32))
    return jnp.concatenate(rows, axis=0).T.astype(BF16)


def stack_right(scaled):
    high, middle, low = split3(-2.0 * scaled)
    n_high, n_middle, n_low, one, zero = norm_rows(scaled)
    norms = jnp.concatenate([one, one, one, n_high, n_middle, n_low, zero], axis=0)
    rows = [high, middle, high, middle, low, high, norms]
    used = 6 * scaled.shape[0] + 8
    rows.append(jnp.zeros((128 - used, scaled.shape[1]), F32))
    return jnp.concatenate(rows, axis=0).astype(BF16)


def matern3(square):
    square = jnp.maximum(square, 1e-30)
    root = square * lax.rsqrt(square)
    base = root + 1.5
    return (base * base + 0.75) * jnp.exp2(root * (-LOG2E))


def to_row(column):
    shape = (column.shape[0], 128)
    mask = lax.broadcasted_iota(jnp.int32, shape, 0) == lax.broadcasted_iota(jnp.int32, shape, 1)
    return jnp.sum(jnp.where(mask, column, 0.0), axis=0, keepdims=True)


def to_column(row, rows, start=0):
    shape = (rows, 128)
    lane = lax.broadcasted_iota(jnp.int32, shape, 1)
    mask = lane == lax.broadcasted_iota(jnp.int32, shape, 0) + start
    return jnp.sum(jnp.where(mask, row, 0.0), axis=1, keepdims=True)


def row_sum(value):
    return jnp.sum(value, axis=1, keepdims=True)


def each(count, body, init):
    if count <= 16:
        for index in range(count):
            init = body(index, init)
        return init
    return lax.fori_loop(0, count, body, init)


def fill(ref, block):
    def put(index, carry):
        ref[index] = block
        return carry

    each(ref.shape[0], put, 0)


def call(kernel, outs, ins, space=pltpu.VMEM, scratch=(), limit=8, flops=1_000_000, name=None):
    return pl.pallas_call(
        kernel,
        out_shape=[jax.ShapeDtypeStruct(s, d) for s, d in outs],
        in_specs=[pl.BlockSpec(memory_space=space) for _ in ins],
        out_specs=[pl.BlockSpec(memory_space=pltpu.VMEM) for _ in outs],
        scratch_shapes=list(scratch),
        compiler_params=pltpu.CompilerParams(vmem_limit_bytes=limit * MIB),
        cost_estimate=pl.CostEstimate(flops=flops, bytes_accessed=1 << 20, transcendentals=0),
        name=name,
    )(*ins)


def prepare_kernel(
    points_hbm, rhs_hbm, basis_hbm, lift_hbm, noise_hbm, scale_hbm, links_hbm, skel_hbm,
    beside_ref, send_ref, weight_ref,
    points_ref, rhs_ref, basis_ref, lift_ref, noise_ref, scale_ref, links_ref, skel_ref, sems,
):
    sources = (points_hbm, scale_hbm, links_hbm, rhs_hbm, basis_hbm, skel_hbm, lift_hbm, noise_hbm)
    targets = (points_ref, scale_ref, links_ref, rhs_ref, basis_ref, skel_ref, lift_ref, noise_ref)
    copies = [
        pltpu.make_async_copy(source, target, sems.at[index])
        for index, (source, target) in enumerate(zip(sources, targets))
    ]
    for copy in copies:
        copy.start()
    for copy in copies:
        copy.wait()
    dim, width = points_ref.shape
    rhs_rows = rhs_ref.shape[0]
    boxes, rows, skel = send_ref.shape
    sub = lax.broadcasted_iota(jnp.int32, (dim, 1), 0)
    scale = jnp.zeros((dim, 1), F32)
    for d in range(dim):
        scale = jnp.where(sub == d, scale_ref[d], scale)
    scaled = points_ref[...] * scale * UNIT
    rhs = rhs_ref[...]
    beside_ref[0:dim, :] = scaled
    beside_ref[dim:, :] = rhs
    lower, upper = links_ref[0, 0].astype(F32), links_ref[0, 1].astype(F32)
    odd = lax.rem(lax.axis_index("leaf"), 2).astype(F32)
    own = 1.0 + lower + upper
    first = odd * lower + (1.0 - odd) * upper
    second = odd * upper + (1.0 - odd) * lower
    sub = lax.broadcasted_iota(jnp.int32, weight_ref.shape, 0)
    weight = jnp.where(sub == 0, own, jnp.where(sub == 1, first, second))
    weight_ref[...] = weight * THIRD
    pick = lax.broadcasted_iota(jnp.int32, (width, skel), 0) == skel_ref[...]
    chosen = fold(raw(triple(scaled), jnp.where(pick, 1.0, 0.0).astype(BF16)))
    coeff = times(rhs, pair(basis_ref[...]))
    lifted = times(coeff, pair(lift_ref[0]))
    square = rhs * rhs
    total = to_row(row_sum(square))
    weighted = to_row(row_sum(square * (noise_ref[...] + own)))
    rest = jnp.zeros((rows - dim - 2 * rhs_rows - 2, skel), F32)
    fill(send_ref, jnp.concatenate([chosen, coeff, lifted, total, weighted, rest], axis=0))


def near_kernel(weight_ref, own_ref, other_ref, vec_ref, out_ref, *, kind):
    rhs_rows, width = out_ref.shape
    dim = own_ref.shape[0] - rhs_rows
    start = vec_ref.shape[0] - rhs_rows
    block = min(256, width)
    left = stack_left(other_ref[0:dim, :])
    right = stack_right(own_ref[0:dim, :])
    vec = triple(vec_ref[start:, :])
    weight = weight_ref[kind : kind + 1, 0:1]
    for c in range(width // block):
        cols = slice(c * block, (c + 1) * block)
        total = jnp.zeros((3 * rhs_rows, block), F32)
        for i in range(width // block):
            rows = slice(i * block, (i + 1) * block)
            high, low = split2(matern3(raw(left[rows], right[:, cols])))
            total = total + raw(vec[:, rows], high) + raw(vec[:, rows], low)
        out_ref[:, cols] = fold(total) * weight


def group_kernel(got_ref, pick_ref, out_ref, *, dim, rhs_rows):
    boxes, rows, skel = got_ref.shape
    start = dim + rhs_rows

    def body(index, carry):
        chosen, summed = carry
        block = got_ref[index]
        pick = lax.broadcasted_iota(jnp.int32, (skel, skel), 0) + index * skel == pick_ref[...]
        pick = jnp.where(pick, 1.0, 0.0).astype(BF16)
        return chosen + raw(triple(block[0:dim]), pick), summed + block[start:]

    zero = (jnp.zeros((3 * dim, skel), F32), jnp.zeros((rows - start, skel), F32))
    chosen, summed = each(boxes, body, zero)
    out_ref[0:dim, :] = fold(chosen)
    out_ref[dim:, :] = summed


def box_chunks(boxes):
    step = min(boxes, 16)
    while boxes % step:
        step -= 1
    return step, boxes // step


def far_kernel(got_ref, mine_ref, high_ref, low_ref, out_ref, *, dim):
    rhs_rows, skel = out_ref.shape
    step, count = box_chunks(got_ref.shape[0])
    left = stack_left(mine_ref[0, 0:dim, :])

    def body(index, total):
        blocks = [got_ref[index * step + j] for j in range(step)]
        right = stack_right(jnp.concatenate([block[0:dim] for block in blocks], axis=1))
        coeff = jnp.concatenate([block[dim : dim + rhs_rows] for block in blocks], axis=1)
        high, low = split2(matern3(raw(left, right)))
        high_ref[index] = high
        low_ref[index] = low
        return total + times_parts_t(coeff, high, low)

    out_ref[...] = each(count, body, jnp.zeros((rhs_rows, skel), F32)) * THIRD


def far_again_kernel(got_ref, high_ref, low_ref, out_ref):
    rhs_rows, skel = out_ref.shape
    step, count = box_chunks(got_ref.shape[0])

    def body(index, total):
        blocks = [got_ref[index * step + j, 0:rhs_rows, :] for j in range(step)]
        coeff = jnp.concatenate(blocks, axis=1)
        return total + times_parts_t(coeff, high_ref[index], low_ref[index])

    out_ref[...] = each(count, body, jnp.zeros((rhs_rows, skel), F32)) * THIRD


def sum_kernel(got_ref, out_ref):
    start = got_ref.shape[1] - out_ref.shape[0]

    def body(index, total):
        return total + got_ref[index, start:, :]

    out_ref[...] = each(got_ref.shape[0], body, jnp.zeros(out_ref.shape, F32))


def first_image_kernel(*refs, dim, groups):
    group_refs = refs[0:groups]
    (far_ref, near_ref, near_a_ref, near_b_ref, rhs_ref, noise_ref, lift_ref, basis_ref,
     shift_ref, sigma_ref, send_ref, high_ref, low_ref) = refs[groups:]
    rhs_rows = rhs_ref.shape[0]
    boxes, rows, skel = send_ref.shape
    left = stack_left(group_refs[0][0:dim, :])
    right = stack_right(jnp.concatenate([ref[0:dim, :] for ref in group_refs], axis=1))
    high, low = split2(matern3(raw(left, right)))
    high_ref[...] = high
    low_ref[...] = low
    start = dim + rhs_rows
    coeff = jnp.concatenate([ref[dim:start, :] for ref in group_refs], axis=1)
    top = times_parts_t(coeff, high, low) * THIRD
    sums = sum(ref[start : start + 8, :] for ref in group_refs)
    total = to_column(sums[0:1], rhs_rows)
    sigma = to_column(sums[1:2], rhs_rows) / jnp.maximum(total, 1e-30)
    rhs = rhs_ref[...]
    basis = pair(basis_ref[...])
    lift = pair(lift_ref[0])
    row = far_ref[...] + times_t(top, lift)
    near = near_ref[...] + near_a_ref[...] + near_b_ref[...]
    shift = (noise_ref[...] - sigma) * rhs + near + times_t(row, basis)
    shift_ref[...] = shift
    lane = lax.broadcasted_iota(jnp.int32, sigma_ref.shape, 1)
    sigma_ref[...] = jnp.where(lane == 0, sigma, total)
    coeff = times(shift, basis)
    lifted = times(coeff, lift)
    curve = to_row(row_sum(rhs * shift))
    rest = jnp.zeros((rows - 2 * rhs_rows - 1, skel), F32)
    fill(send_ref, jnp.concatenate([coeff, lifted, curve, rest], axis=0))


def second_image_kernel(*refs, groups):
    group_refs = refs[0:groups]
    (far_ref, near_ref, near_a_ref, near_b_ref, rhs_ref, shift_ref, sigma_ref, noise_ref,
     lift_ref, basis_ref, high_ref, low_ref,
     residual_ref, image_ref, alpha_ref, send_ref) = refs[groups:]
    rhs_rows = rhs_ref.shape[0]
    skel = lift_ref.shape[2]
    coeff = jnp.concatenate([ref[0:rhs_rows, :] for ref in group_refs], axis=1)
    top = times_parts_t(coeff, high_ref[...], low_ref[...]) * THIRD
    sums = sum(ref[rhs_rows : rhs_rows + 8, :] for ref in group_refs)
    along = to_column(sums[0:1], rhs_rows)
    sigma = sigma_ref[:, 0:1]
    total = sigma_ref[:, 1:2]
    curve = along + sigma * total
    alpha = total / curve
    keep = along / curve
    shift = shift_ref[...]
    rhs = rhs_ref[...]
    row = far_ref[...] + times_t(top, pair(lift_ref[0]))
    near = near_ref[...] + near_a_ref[...] + near_b_ref[...]
    second = noise_ref[...] * shift + near + times_t(row, pair(basis_ref[...]))
    residual = keep * rhs - alpha * shift
    image = keep * (shift + sigma * rhs) - alpha * second
    residual_ref[...] = residual
    image_ref[...] = image
    lane = lax.broadcasted_iota(jnp.int32, (rhs_rows, skel), 1)
    index = lax.broadcasted_iota(jnp.int32, (rhs_rows, skel), 0)
    alpha_ref[...] = jnp.where(lane == 0, alpha, jnp.where(lane == 1, total, sigma))
    both = jnp.where(lane == index, row_sum(residual * residual), 0.0)
    both = both + jnp.where(lane == index + rhs_rows, row_sum(residual * image), 0.0)
    fill(send_ref, jnp.sum(both, axis=0, keepdims=True))


def finish_kernel(
    got_ref, alpha_ref, rhs_ref, shift_ref, residual_ref, image_ref, solution_ref, out_ref
):
    rhs_rows = rhs_ref.shape[0]
    sums = jnp.sum(got_ref[...], axis=0)
    norm_next = to_column(sums, rhs_rows)
    curve = to_column(sums, rhs_rows, rhs_rows)
    alpha = alpha_ref[:, 0:1]
    norm_now = alpha_ref[:, 1:2]
    ratio = norm_next / norm_now
    step = norm_next / (curve - ratio * norm_next / alpha)
    rhs = rhs_ref[...]
    residual = residual_ref[...]
    image = shift_ref[...] + alpha_ref[:, 2:3] * rhs
    solution_ref[...] = alpha * rhs + step * (residual + ratio * rhs)
    out_ref[...] = residual - step * (image_ref[...] + ratio * image)


def spread(value, axis):
    return lax.all_to_all(value, axis, 0, 0, tiled=True)


def local(points, rhs, basis, transfer, noise, inv_scale, links, leaf_skel, group_skel):
    dim, width = points.shape
    rhs_rows = rhs.shape[0]
    skel = basis.shape[1]
    boxes = lax.axis_size("leaf")
    groups = lax.axis_size("grp")
    noise = noise[None, :]
    pairs_a = [(i, i ^ 1) for i in range(boxes) if (i ^ 1) < boxes]
    pairs_b = [(i, ((i + 1) ^ 1) - 1) for i in range(boxes) if 0 <= ((i + 1) ^ 1) - 1 < boxes]
    wide = (rhs_rows, width)
    small = (rhs_rows, skel)
    step, count = box_chunks(boxes)

    rows = -(-(dim + 2 * rhs_rows + 2) // 8) * 8
    inputs = [points, rhs, basis, transfer, noise, inv_scale, links, leaf_skel]
    scratch = [pltpu.VMEM(value.shape, value.dtype) for value in inputs]
    for index in (5, 6):
        scratch[index] = pltpu.SMEM(inputs[index].shape, inputs[index].dtype)
    beside, send, weight = call(
        prepare_kernel,
        [((dim + rhs_rows, width), F32), ((boxes, rows, skel), F32), ((8, skel), F32)],
        inputs, space=pltpu.HBM, scratch=scratch + [pltpu.SemaphoreType.DMA((8,))],
        name="prepare",
    )
    beside_a = lax.ppermute(beside, "leaf", pairs_a)
    beside_b = lax.ppermute(beside, "leaf", pairs_b)
    got = spread(send, "leaf")

    def near_part(other, vec, kind):
        return call(
            functools.partial(near_kernel, kind=kind), [(wide, F32)], [weight, beside, other, vec],
            limit=16, flops=4 * 10**9, name="near",
        )[0]

    near = near_part(beside, beside, 0)
    near_a = near_part(beside_a, beside_a, 1)
    near_b = near_part(beside_b, beside_b, 2)

    def exchange(value):
        return [value] + [
            lax.ppermute(value, "grp", [(i, (i + s) % groups) for i in range(groups)])
            for s in range(1, groups)
        ]

    (mine,) = call(
        functools.partial(group_kernel, dim=dim, rhs_rows=rhs_rows),
        [((rows - rhs_rows, skel), F32)], [got, group_skel], name="group",
    )
    parts = exchange(mine)
    far_shape = ((count, skel, step * skel), BF16)
    far_high, far_low, far = call(
        functools.partial(far_kernel, dim=dim), [far_shape, far_shape, (small, F32)], [got, send],
        limit=16, flops=10**9, name="far",
    )
    rows_next = -(-(2 * rhs_rows + 1) // 8) * 8
    top_shape = ((skel, groups * skel), BF16)
    shift, sigma, send, top_high, top_low = call(
        functools.partial(first_image_kernel, dim=dim, groups=groups),
        [(wide, F32), (small, F32), ((boxes, rows_next, skel), F32), top_shape, top_shape],
        [*parts, far, near, near_a, near_b, rhs, noise, transfer, basis], name="image",
    )
    shift_a = lax.ppermute(shift, "leaf", pairs_a)
    shift_b = lax.ppermute(shift, "leaf", pairs_b)
    got = spread(send, "leaf")
    near = near_part(beside, shift, 0)
    near_a = near_part(beside_a, shift_a, 1)
    near_b = near_part(beside_b, shift_b, 2)
    (mine,) = call(sum_kernel, [((rows_next - rhs_rows, skel), F32)], [got], name="sums")
    parts = exchange(mine)
    (far,) = call(
        far_again_kernel, [(small, F32)], [got, far_high, far_low], flops=10**8, name="faragain"
    )
    residual, image, alpha, send = call(
        functools.partial(second_image_kernel, groups=groups),
        [(wide, F32), (wide, F32), (small, F32), ((boxes * groups, 1, skel), F32)],
        [*parts, far, near, near_a, near_b, rhs, shift, sigma, noise, transfer, basis,
         top_high, top_low],
        name="second",
    )
    got = spread(send, ("grp", "leaf"))
    return tuple(
        call(
            finish_kernel, [(wide, F32), (wide, F32)],
            [got, alpha, rhs, shift, residual, image], name="finish",
        )
    )


def solution(mesh):
    return jax.shard_map(
        local,
        mesh=mesh,
        in_specs=(
            P(None, ("grp", "leaf")),
            P(None, ("grp", "leaf")),
            P(("grp", "leaf"), None),
            P(("grp", "leaf"), None, None),
            P(("grp", "leaf")),
            P(),
            P(("grp", "leaf"), None),
            P(("grp", "leaf"), None),
            P("grp", None),
        ),
        out_specs=(P(None, ("grp", "leaf")), P(None, ("grp", "leaf"))),
        check_vma=False,
    )
```

```python
import functools
import math

import jax
import jax.numpy as jnp
from jax import lax
from jax.experimental import pallas as pl
from jax.experimental.pallas import tpu as pltpu
from jax.sharding import PartitionSpec as P


F32 = jnp.float32
BF16 = jnp.bfloat16
LOG2E = math.log2(math.e)
UNIT = math.sqrt(5.0)
THIRD = 1.0 / 3.0
MIB = 1 << 20
SHIFT = 3.0


def raw(first, second):
    return lax.dot_general(
        first, second, (((1,), (0,)), ((), ())), preferred_element_type=F32
    )


def raw_t(first, second):
    return lax.dot_general(
        first, second, (((1,), (1,)), ((), ())), preferred_element_type=F32
    )


def split3(value):
    high = value.astype(BF16).astype(F32)
    rest = value - high
    middle = rest.astype(BF16).astype(F32)
    return high, middle, (rest - middle).astype(BF16).astype(F32)


def split2(value):
    high = value.astype(BF16)
    return high, (value - high.astype(F32)).astype(BF16)


def triple(value):
    return jnp.concatenate(split3(value), axis=0).astype(BF16)


def fold(value):
    rows = value.shape[0] // 3
    return value[0:rows] + value[rows : 2 * rows] + value[2 * rows :]


def pair(value):
    return jnp.concatenate(split2(value), axis=1)


def times(first, second):
    half = second.shape[1] // 2
    both = fold(raw(triple(first), second))
    return both[:, :half] + both[:, half:]


def times_t(first, second):
    parts = triple(first)
    return fold(raw_t(jnp.concatenate([parts, parts], axis=1), second))


def times_parts_t(first, high, low):
    parts = triple(first)
    return fold(raw_t(parts, high) + raw_t(parts, low))


def norm_rows(scaled):
    high, middle, low = split3(jnp.sum(scaled * scaled, axis=0, keepdims=True))
    one = jnp.ones_like(high)
    zero = jnp.zeros((2,) + high.shape[1:], F32)
    return high, middle, low, one, zero


def stack_left(scaled):
    high, middle, low = split3(scaled)
    n_high, n_middle, n_low, one, zero = norm_rows(scaled)
    norms = jnp.concatenate([n_high, n_middle, n_low, one, one, one, zero], axis=0)
    rows = [high, high, middle, middle, high, low, norms]
    used = 6 * scaled.shape[0] + 8
    rows.append(jnp.zeros((128 - used, scaled.shape[1]), F32))
    return jnp.concatenate(rows, axis=0).T.astype(BF16)


def stack_right(scaled):
    high, middle, low = split3(-2.0 * scaled)
    n_high, n_middle, n_low, one, zero = norm_rows(scaled)
    norms = jnp.concatenate([one, one, one, n_high, n_middle, n_low, zero], axis=0)
    rows = [high, middle, high, middle, low, high, norms]
    used = 6 * scaled.shape[0] + 8
    rows.append(jnp.zeros((128 - used, scaled.shape[1]), F32))
    return jnp.concatenate(rows, axis=0).astype(BF16)


def matern3(square):
    square = jnp.maximum(square, 1e-30)
    root = square * lax.rsqrt(square)
    base = root + 1.5
    return (base * base + 0.75) * jnp.exp2(root * (-LOG2E))


def to_row(column):
    shape = (column.shape[0], 128)
    mask = lax.broadcasted_iota(jnp.int32, shape, 0) == lax.broadcasted_iota(jnp.int32, shape, 1)
    return jnp.sum(jnp.where(mask, column, 0.0), axis=0, keepdims=True)


def to_column(row, rows, start=0):
    shape = (rows, 128)
    lane = lax.broadcasted_iota(jnp.int32, shape, 1)
    mask = lane == lax.broadcasted_iota(jnp.int32, shape, 0) + start
    return jnp.sum(jnp.where(mask, row, 0.0), axis=1, keepdims=True)


def row_sum(value):
    return jnp.sum(value, axis=1, keepdims=True)


def each(count, body, init):
    if count <= 16:
        for index in range(count):
            init = body(index, init)
        return init
    return lax.fori_loop(0, count, body, init)


def fill(ref, block):
    def put(index, carry):
        ref[index] = block
        return carry

    each(ref.shape[0], put, 0)


def call(kernel, outs, ins, space=pltpu.VMEM, scratch=(), limit=8, flops=1_000_000):
    return pl.pallas_call(
        kernel,
        out_shape=[jax.ShapeDtypeStruct(s, d) for s, d in outs],
        in_specs=[pl.BlockSpec(memory_space=space) for _ in ins],
        out_specs=[pl.BlockSpec(memory_space=pltpu.VMEM) for _ in outs],
        scratch_shapes=list(scratch),
        compiler_params=pltpu.CompilerParams(vmem_limit_bytes=limit * MIB),
        cost_estimate=pl.CostEstimate(flops=flops, bytes_accessed=1 << 20, transcendentals=0),
    )(*ins)


def prepare_kernel(
    points_hbm, rhs_hbm, basis_hbm, lift_hbm, noise_hbm, scale_hbm, links_hbm, skel_hbm,
    beside_ref, send_ref, weight_ref,
    points_ref, rhs_ref, basis_ref, lift_ref, noise_ref, scale_ref, links_ref, skel_ref, sems,
):
    sources = (points_hbm, scale_hbm, links_hbm, rhs_hbm, basis_hbm, skel_hbm, lift_hbm, noise_hbm)
    targets = (points_ref, scale_ref, links_ref, rhs_ref, basis_ref, skel_ref, lift_ref, noise_ref)
    copies = [
        pltpu.make_async_copy(source, target, sems.at[index])
        for index, (source, target) in enumerate(zip(sources, targets))
    ]
    for copy in copies:
        copy.start()
    for copy in copies:
        copy.wait()
    dim, width = points_ref.shape
    rhs_rows = rhs_ref.shape[0]
    _, rows, skel = send_ref.shape
    sub = lax.broadcasted_iota(jnp.int32, (dim, 1), 0)
    scale = jnp.zeros((dim, 1), F32)
    for d in range(dim):
        scale = jnp.where(sub == d, scale_ref[d], scale)
    scaled = points_ref[...] * scale * UNIT
    rhs = rhs_ref[...]
    beside_ref[0:dim, :] = scaled
    beside_ref[dim:, :] = rhs
    lower, upper = links_ref[0, 0].astype(F32), links_ref[0, 1].astype(F32)
    odd = lax.rem(lax.axis_index("leaf"), 2).astype(F32)
    own = 1.0 + lower + upper
    first = odd * lower + (1.0 - odd) * upper
    second = odd * upper + (1.0 - odd) * lower
    sub = lax.broadcasted_iota(jnp.int32, weight_ref.shape, 0)
    weight = jnp.where(sub == 0, own, jnp.where(sub == 1, first, second))
    weight_ref[...] = weight * THIRD
    pick = lax.broadcasted_iota(jnp.int32, (width, skel), 0) == skel_ref[...]
    chosen = fold(raw(triple(scaled), jnp.where(pick, 1.0, 0.0).astype(BF16)))
    coeff = times(rhs, pair(basis_ref[...]))
    lifted = times(coeff, pair(lift_ref[0]))
    parts = [chosen, coeff, lifted]
    if rows > dim + 2 * rhs_rows:
        parts.append(jnp.zeros((rows - dim - 2 * rhs_rows, skel), F32))
    fill(send_ref, jnp.concatenate(parts, axis=0))


def near_kernel(weight_ref, own_ref, other_ref, vec_ref, out_ref, *, kind):
    rhs_rows, width = out_ref.shape
    dim = own_ref.shape[0] - rhs_rows
    start = vec_ref.shape[0] - rhs_rows
    block = min(256, width)
    left = stack_left(other_ref[0:dim, :])
    right = stack_right(own_ref[0:dim, :])
    vec = triple(vec_ref[start:, :])
    weight = weight_ref[kind : kind + 1, 0:1]
    for c in range(width // block):
        cols = slice(c * block, (c + 1) * block)
        total = jnp.zeros((3 * rhs_rows, block), F32)
        for i in range(width // block):
            rows = slice(i * block, (i + 1) * block)
            high, low = split2(matern3(raw(left[rows], right[:, cols])))
            total = total + raw(vec[:, rows], high) + raw(vec[:, rows], low)
        out_ref[:, cols] = fold(total) * weight


def group_kernel(got_ref, pick_ref, out_ref, *, dim, rhs_rows):
    boxes, rows, skel = got_ref.shape
    start = dim + rhs_rows

    def body(index, carry):
        chosen, summed = carry
        block = got_ref[index]
        pick = lax.broadcasted_iota(jnp.int32, (skel, skel), 0) + index * skel == pick_ref[...]
        pick = jnp.where(pick, 1.0, 0.0).astype(BF16)
        return chosen + raw(triple(block[0:dim]), pick), summed + block[start:]

    zero = (jnp.zeros((3 * dim, skel), F32), jnp.zeros((rows - start, skel), F32))
    chosen, summed = each(boxes, body, zero)
    out_ref[0:dim, :] = fold(chosen)
    out_ref[dim:, :] = summed


def box_chunks(boxes):
    step = min(boxes, 16)
    while boxes % step:
        step -= 1
    return step, boxes // step


def far_kernel(got_ref, mine_ref, high_ref, low_ref, out_ref, *, dim):
    rhs_rows, skel = out_ref.shape
    step, count = box_chunks(got_ref.shape[0])
    left = stack_left(mine_ref[0, 0:dim, :])

    def body(index, total):
        blocks = [got_ref[index * step + j] for j in range(step)]
        right = stack_right(jnp.concatenate([block[0:dim] for block in blocks], axis=1))
        coeff = jnp.concatenate([block[dim : dim + rhs_rows] for block in blocks], axis=1)
        high, low = split2(matern3(raw(left, right)))
        high_ref[index] = high
        low_ref[index] = low
        return total + times_parts_t(coeff, high, low)

    out_ref[...] = each(count, body, jnp.zeros((rhs_rows, skel), F32)) * THIRD


def far_again_kernel(got_ref, high_ref, low_ref, out_ref):
    rhs_rows, skel = out_ref.shape
    step, count = box_chunks(got_ref.shape[0])

    def body(index, total):
        blocks = [got_ref[index * step + j, 0:rhs_rows, :] for j in range(step)]
        coeff = jnp.concatenate(blocks, axis=1)
        return total + times_parts_t(coeff, high_ref[index], low_ref[index])

    out_ref[...] = each(count, body, jnp.zeros((rhs_rows, skel), F32)) * THIRD


def sum_kernel(got_ref, out_ref):
    start = got_ref.shape[1] - out_ref.shape[0]

    def body(index, total):
        return total + got_ref[index, start:, :]

    out_ref[...] = each(got_ref.shape[0], body, jnp.zeros(out_ref.shape, F32))


def first_image_kernel(*refs, dim, groups):
    group_refs = refs[0:groups]
    (far_ref, near_ref, near_a_ref, near_b_ref, rhs_ref, noise_ref, lift_ref, basis_ref,
     shift_ref, send_ref, high_ref, low_ref) = refs[groups:]
    rhs_rows = rhs_ref.shape[0]
    _, rows, skel = send_ref.shape
    left = stack_left(group_refs[0][0:dim, :])
    right = stack_right(jnp.concatenate([ref[0:dim, :] for ref in group_refs], axis=1))
    high, low = split2(matern3(raw(left, right)))
    high_ref[...] = high
    low_ref[...] = low
    start = dim + rhs_rows
    coeff = jnp.concatenate([ref[dim:start, :] for ref in group_refs], axis=1)
    top = times_parts_t(coeff, high, low) * THIRD
    rhs = rhs_ref[...]
    basis = pair(basis_ref[...])
    lift = pair(lift_ref[0])
    row = far_ref[...] + times_t(top, lift)
    near = near_ref[...] + near_a_ref[...] + near_b_ref[...]
    shift = (noise_ref[...] - SHIFT) * rhs + near + times_t(row, basis)
    shift_ref[...] = shift
    coeff = times(shift, basis)
    lifted = times(coeff, lift)
    total = to_row(row_sum(rhs * rhs))
    along = to_row(row_sum(rhs * shift))
    rest = jnp.zeros((rows - 2 * rhs_rows - 2, skel), F32)
    fill(send_ref, jnp.concatenate([coeff, lifted, total, along, rest], axis=0))


def second_image_kernel(*refs, groups):
    group_refs = refs[0:groups]
    (far_ref, near_ref, near_a_ref, near_b_ref, rhs_ref, shift_ref, noise_ref,
     lift_ref, basis_ref, high_ref, low_ref,
     residual_ref, image_ref, alpha_ref, send_ref) = refs[groups:]
    rhs_rows = rhs_ref.shape[0]
    skel = lift_ref.shape[2]
    coeff = jnp.concatenate([ref[0:rhs_rows, :] for ref in group_refs], axis=1)
    top = times_parts_t(coeff, high_ref[...], low_ref[...]) * THIRD
    sums = sum(ref[rhs_rows : rhs_rows + 8, :] for ref in group_refs)
    total = to_column(sums[0:1], rhs_rows)
    along = to_column(sums[1:2], rhs_rows)
    curve = along + SHIFT * total
    alpha = total / curve
    keep = along / curve
    shift = shift_ref[...]
    rhs = rhs_ref[...]
    row = far_ref[...] + times_t(top, pair(lift_ref[0]))
    near = near_ref[...] + near_a_ref[...] + near_b_ref[...]
    second = noise_ref[...] * shift + near + times_t(row, pair(basis_ref[...]))
    residual = keep * rhs - alpha * shift
    image = keep * (shift + SHIFT * rhs) - alpha * second
    residual_ref[...] = residual
    image_ref[...] = image
    lane = lax.broadcasted_iota(jnp.int32, (rhs_rows, skel), 1)
    index = lax.broadcasted_iota(jnp.int32, (rhs_rows, skel), 0)
    alpha_ref[...] = jnp.where(lane == 0, alpha, total)
    both = jnp.where(lane == index, row_sum(residual * residual), 0.0)
    both = both + jnp.where(lane == index + rhs_rows, row_sum(residual * image), 0.0)
    fill(send_ref, jnp.sum(both, axis=0, keepdims=True))


def finish_kernel(
    got_ref, alpha_ref, rhs_ref, shift_ref, residual_ref, image_ref, solution_ref, out_ref
):
    rhs_rows = rhs_ref.shape[0]
    sums = jnp.sum(got_ref[...], axis=0)
    norm_next = to_column(sums, rhs_rows)
    curve = to_column(sums, rhs_rows, rhs_rows)
    alpha = alpha_ref[:, 0:1]
    norm_now = alpha_ref[:, 1:2]
    ratio = norm_next / norm_now
    step = norm_next / (curve - ratio * norm_next / alpha)
    rhs = rhs_ref[...]
    residual = residual_ref[...]
    image = shift_ref[...] + SHIFT * rhs
    solution_ref[...] = alpha * rhs + step * (residual + ratio * rhs)
    out_ref[...] = residual - step * (image_ref[...] + ratio * image)


def spread(value, axis):
    return lax.all_to_all(value, axis, 0, 0, tiled=True)


def pass_on(value, pairs):
    return lax.ppermute(value, "leaf", pairs)


def local(points, rhs, basis, transfer, noise, inv_scale, links, leaf_skel, group_skel):
    dim, width = points.shape
    rhs_rows = rhs.shape[0]
    skel = basis.shape[1]
    boxes = lax.axis_size("leaf")
    groups = lax.axis_size("grp")
    noise = noise[None, :]
    pairs_a = [(i, i ^ 1) for i in range(boxes) if (i ^ 1) < boxes]
    pairs_b = [(i, ((i + 1) ^ 1) - 1) for i in range(boxes) if 0 <= ((i + 1) ^ 1) - 1 < boxes]
    wide = (rhs_rows, width)
    small = (rhs_rows, skel)
    step, count = box_chunks(boxes)

    rows = -(-(dim + 2 * rhs_rows) // 8) * 8
    inputs = [points, rhs, basis, transfer, noise, inv_scale, links, leaf_skel]
    scratch = [pltpu.VMEM(value.shape, value.dtype) for value in inputs]
    for index in (5, 6):
        scratch[index] = pltpu.SMEM(inputs[index].shape, inputs[index].dtype)
    beside, send, weight = call(
        prepare_kernel,
        [((dim + rhs_rows, width), F32), ((boxes, rows, skel), F32), ((8, skel), F32)],
        inputs, space=pltpu.HBM, scratch=scratch + [pltpu.SemaphoreType.DMA((8,))],
        limit=60,
    )
    got = spread(send, "leaf")
    beside_a = pass_on(beside, pairs_a)
    beside_b = pass_on(beside, pairs_b)

    def near_part(other, vec, kind):
        return call(
            functools.partial(near_kernel, kind=kind), [(wide, F32)],
            [weight, beside, other, vec], limit=16, flops=4 * 10**9,
        )[0]

    near = near_part(beside, beside, 0)
    near_a = near_part(beside_a, beside_a, 1)
    near_b = near_part(beside_b, beside_b, 2)

    def exchange(value):
        return [value] + [
            lax.ppermute(value, "grp", [(i, (i + s) % groups) for i in range(groups)])
            for s in range(1, groups)
        ]

    (mine,) = call(
        functools.partial(group_kernel, dim=dim, rhs_rows=rhs_rows),
        [((rows - rhs_rows, skel), F32)], [got, group_skel],
    )
    parts = exchange(mine)
    far_shape = ((count, skel, step * skel), BF16)
    far_high, far_low, far = call(
        functools.partial(far_kernel, dim=dim), [far_shape, far_shape, (small, F32)], [got, send],
        limit=16, flops=10**9,
    )
    rows_next = -(-(2 * rhs_rows + 2) // 8) * 8
    top_shape = ((skel, groups * skel), BF16)
    shift, send, top_high, top_low = call(
        functools.partial(first_image_kernel, dim=dim, groups=groups),
        [(wide, F32), ((boxes, rows_next, skel), F32), top_shape, top_shape],
        [*parts, far, near, near_a, near_b, rhs, noise, transfer, basis],
    )
    got = spread(send, "leaf")
    shift_a = pass_on(shift, pairs_a)
    shift_b = pass_on(shift, pairs_b)
    near = near_part(beside, shift, 0)
    near_a = near_part(beside_a, shift_a, 1)
    near_b = near_part(beside_b, shift_b, 2)
    (mine,) = call(sum_kernel, [((rows_next - rhs_rows, skel), F32)], [got])
    parts = exchange(mine)
    (far,) = call(far_again_kernel, [(small, F32)], [got, far_high, far_low], flops=10**8)
    residual, image, alpha, send = call(
        functools.partial(second_image_kernel, groups=groups),
        [(wide, F32), (wide, F32), (small, F32), ((boxes * groups, 1, skel), F32)],
        [*parts, far, near, near_a, near_b, rhs, shift, noise, transfer, basis,
         top_high, top_low],
    )
    got = spread(send, ("grp", "leaf"))
    return tuple(
        call(
            finish_kernel, [(wide, F32), (wide, F32)],
            [got, alpha, rhs, shift, residual, image],
        )
    )


def solution(mesh):
    return jax.shard_map(
        local,
        mesh=mesh,
        in_specs=(
            P(None, ("grp", "leaf")),
            P(None, ("grp", "leaf")),
            P(("grp", "leaf"), None),
            P(("grp", "leaf"), None, None),
            P(("grp", "leaf")),
            P(),
            P(("grp", "leaf"), None),
            P(("grp", "leaf"), None),
            P("grp", None),
        ),
        out_specs=(P(None, ("grp", "leaf")), P(None, ("grp", "leaf"))),
        check_vma=False,
    )
```

```python
import functools
import math

import jax
import jax.numpy as jnp
from jax import lax
from jax.experimental import pallas as pl
from jax.experimental.pallas import tpu as pltpu
from jax.sharding import PartitionSpec as P


F32 = jnp.float32
BF16 = jnp.bfloat16
LOG2E = math.log2(math.e)
UNIT = math.sqrt(5.0)
THIRD = 1.0 / 3.0
MIB = 1 << 20
SHIFT = 3.0


def raw(first, second):
    return lax.dot_general(
        first, second, (((1,), (0,)), ((), ())), preferred_element_type=F32
    )


def raw_t(first, second):
    return lax.dot_general(
        first, second, (((1,), (1,)), ((), ())), preferred_element_type=F32
    )


def split3(value):
    high = value.astype(BF16).astype(F32)
    rest = value - high
    middle = rest.astype(BF16).astype(F32)
    return high, middle, (rest - middle).astype(BF16).astype(F32)


def split2(value):
    high = value.astype(BF16)
    return high, (value - high.astype(F32)).astype(BF16)


def triple(value):
    return jnp.concatenate(split3(value), axis=0).astype(BF16)


def fold(value):
    rows = value.shape[0] // 3
    return value[0:rows] + value[rows : 2 * rows] + value[2 * rows :]


def pair(value):
    return jnp.concatenate(split2(value), axis=1)


def times(first, second):
    half = second.shape[1] // 2
    both = fold(raw(triple(first), second))
    return both[:, :half] + both[:, half:]


def times_t(first, second):
    parts = triple(first)
    return fold(raw_t(jnp.concatenate([parts, parts], axis=1), second))


def times_parts_t(first, high, low):
    parts = triple(first)
    return fold(raw_t(parts, high) + raw_t(parts, low))


def norm_rows(scaled):
    high, middle, low = split3(jnp.sum(scaled * scaled, axis=0, keepdims=True))
    one = jnp.ones_like(high)
    zero = jnp.zeros((2,) + high.shape[1:], F32)
    return high, middle, low, one, zero


def stack_left(scaled):
    high, middle, low = split3(scaled)
    n_high, n_middle, n_low, one, zero = norm_rows(scaled)
    norms = jnp.concatenate([n_high, n_middle, n_low, one, one, one, zero], axis=0)
    rows = [high, high, middle, middle, high, low, norms]
    used = 6 * scaled.shape[0] + 8
    rows.append(jnp.zeros((128 - used, scaled.shape[1]), F32))
    return jnp.concatenate(rows, axis=0).T.astype(BF16)


def stack_right(scaled):
    high, middle, low = split3(-2.0 * scaled)
    n_high, n_middle, n_low, one, zero = norm_rows(scaled)
    norms = jnp.concatenate([one, one, one, n_high, n_middle, n_low, zero], axis=0)
    rows = [high, middle, high, middle, low, high, norms]
    used = 6 * scaled.shape[0] + 8
    rows.append(jnp.zeros((128 - used, scaled.shape[1]), F32))
    return jnp.concatenate(rows, axis=0).astype(BF16)


def matern3(square):
    square = jnp.maximum(square, 1e-30)
    root = square * lax.rsqrt(square)
    base = root + 1.5
    return (base * base + 0.75) * jnp.exp2(root * (-LOG2E))


def to_row(column):
    shape = (column.shape[0], 128)
    mask = lax.broadcasted_iota(jnp.int32, shape, 0) == lax.broadcasted_iota(jnp.int32, shape, 1)
    return jnp.sum(jnp.where(mask, column, 0.0), axis=0, keepdims=True)


def to_column(row, rows, start=0):
    shape = (rows, 128)
    lane = lax.broadcasted_iota(jnp.int32, shape, 1)
    mask = lane == lax.broadcasted_iota(jnp.int32, shape, 0) + start
    return jnp.sum(jnp.where(mask, row, 0.0), axis=1, keepdims=True)


def row_sum(value):
    return jnp.sum(value, axis=1, keepdims=True)


def each(count, body, init):
    if count <= 16:
        for index in range(count):
            init = body(index, init)
        return init
    return lax.fori_loop(0, count, body, init)


def fill(ref, block):
    def put(index, carry):
        ref[index] = block
        return carry

    each(ref.shape[0], put, 0)


def call(kernel, outs, ins, space=pltpu.VMEM, scratch=(), limit=8, flops=1_000_000):
    return pl.pallas_call(
        kernel,
        out_shape=[jax.ShapeDtypeStruct(s, d) for s, d in outs],
        in_specs=[pl.BlockSpec(memory_space=space) for _ in ins],
        out_specs=[pl.BlockSpec(memory_space=pltpu.VMEM) for _ in outs],
        scratch_shapes=list(scratch),
        compiler_params=pltpu.CompilerParams(vmem_limit_bytes=limit * MIB),
        cost_estimate=pl.CostEstimate(flops=flops, bytes_accessed=1 << 20, transcendentals=0),
    )(*ins)


def prepare_kernel(
    points_hbm, rhs_hbm, basis_hbm, lift_hbm, noise_hbm, scale_hbm, links_hbm, skel_hbm,
    beside_ref, send_ref, weight_ref,
    points_ref, rhs_ref, basis_ref, lift_ref, noise_ref, scale_ref, links_ref, skel_ref, sems,
):
    sources = (points_hbm, scale_hbm, links_hbm, rhs_hbm, basis_hbm, skel_hbm, lift_hbm, noise_hbm)
    targets = (points_ref, scale_ref, links_ref, rhs_ref, basis_ref, skel_ref, lift_ref, noise_ref)
    copies = [
        pltpu.make_async_copy(source, target, sems.at[index])
        for index, (source, target) in enumerate(zip(sources, targets))
    ]
    for copy in copies:
        copy.start()
    for copy in copies:
        copy.wait()
    dim, width = points_ref.shape
    rhs_rows = rhs_ref.shape[0]
    rows, skel = send_ref.shape[1:]
    sub = lax.broadcasted_iota(jnp.int32, (dim, 1), 0)
    scale = jnp.zeros((dim, 1), F32)
    for d in range(dim):
        scale = jnp.where(sub == d, scale_ref[d], scale)
    scaled = points_ref[...] * scale * UNIT
    rhs = rhs_ref[...]
    beside_ref[0:dim, :] = scaled
    beside_ref[dim:, :] = rhs
    lower, upper = links_ref[0, 0].astype(F32), links_ref[0, 1].astype(F32)
    odd = lax.rem(lax.axis_index("leaf"), 2).astype(F32)
    own = 1.0 + lower + upper
    first = odd * lower + (1.0 - odd) * upper
    second = odd * upper + (1.0 - odd) * lower
    sub = lax.broadcasted_iota(jnp.int32, weight_ref.shape, 0)
    weight = jnp.where(sub == 0, own, jnp.where(sub == 1, first, second))
    weight_ref[...] = weight * THIRD
    pick = lax.broadcasted_iota(jnp.int32, (width, skel), 0) == skel_ref[...]
    chosen = fold(raw(triple(scaled), jnp.where(pick, 1.0, 0.0).astype(BF16)))
    coeff = times(rhs, pair(basis_ref[...]))
    lifted = times(coeff, pair(lift_ref[0]))
    parts = [chosen, coeff, lifted]
    if rows > dim + 2 * rhs_rows:
        parts.append(jnp.zeros((rows - dim - 2 * rhs_rows, skel), F32))
    fill(send_ref, jnp.concatenate(parts, axis=0))


def near_kernel(weight_ref, own_ref, other_ref, vec_ref, out_ref, *, kind):
    rhs_rows, width = out_ref.shape
    dim = own_ref.shape[0] - rhs_rows
    start = vec_ref.shape[0] - rhs_rows
    block = min(256, width)
    left = stack_left(other_ref[0:dim, :])
    right = stack_right(own_ref[0:dim, :])
    vec = triple(vec_ref[start:, :])
    weight = weight_ref[kind : kind + 1, 0:1]
    for c in range(width // block):
        cols = slice(c * block, (c + 1) * block)
        total = jnp.zeros((3 * rhs_rows, block), F32)
        for i in range(width // block):
            rows = slice(i * block, (i + 1) * block)
            high, low = split2(matern3(raw(left[rows], right[:, cols])))
            total = total + raw(vec[:, rows], high) + raw(vec[:, rows], low)
        out_ref[:, cols] = fold(total) * weight


def box_chunks(boxes):
    step = min(boxes, 16)
    while boxes % step:
        step -= 1
    return step, boxes // step


def picked(ref, pick_refs, swapped, dim, rhs_rows):
    skel = ref.shape[2]
    groups = len(pick_refs)
    half = ref.shape[0] // groups
    parity = lax.rem(lax.axis_index("leaf") + swapped, 2)
    out = []
    for shift, pick_ref in enumerate(pick_refs):
        first = lax.rem(lax.axis_index("grp") + groups - shift, groups) * half

        def body(index, carry, first=first, pick_ref=pick_ref):
            chosen, summed = carry
            block = ref[first + index]
            place = lax.broadcasted_iota(jnp.int32, (skel, skel), 0)
            pick = place + (2 * index + parity) * skel == pick_ref[...]
            pick = jnp.where(pick, 1.0, 0.0).astype(BF16)
            chosen = chosen + raw(triple(block[0:dim]), pick)
            return chosen, summed + block[dim + rhs_rows : dim + 2 * rhs_rows]

        zero = (jnp.zeros((3 * dim, skel), F32), jnp.zeros((rhs_rows, skel), F32))
        chosen, summed = each(half, body, zero)
        out.append(jnp.concatenate([fold(chosen), summed], axis=0))
    return out


def far_part(ref, groups, left, high_ref, low_ref, dim, rhs_rows):
    skel = ref.shape[2]
    half = ref.shape[0] // groups
    first = lax.axis_index("grp") * half
    step, count = box_chunks(half)

    def body(index, total):
        blocks = [ref[first + index * step + j] for j in range(step)]
        right = stack_right(jnp.concatenate([block[0:dim] for block in blocks], axis=1))
        coeff = jnp.concatenate([block[dim : dim + rhs_rows] for block in blocks], axis=1)
        high, low = split2(matern3(raw(left, right)))
        high_ref[index] = high
        low_ref[index] = low
        return total + times_parts_t(coeff, high, low)

    return each(count, body, jnp.zeros((rhs_rows, skel), F32))


def far_again(ref, groups, high_ref, low_ref, rhs_rows):
    skel = ref.shape[2]
    half = ref.shape[0] // groups
    first = lax.axis_index("grp") * half
    step, count = box_chunks(half)

    def body(index, total):
        blocks = [ref[first + index * step + j, 0:rhs_rows, :] for j in range(step)]
        coeff = jnp.concatenate(blocks, axis=1)
        return total + times_parts_t(coeff, high_ref[index], low_ref[index])

    return each(count, body, jnp.zeros((rhs_rows, skel), F32))


def group_sums(ref, groups, start):
    half = ref.shape[0] // groups
    out = []
    for shift in range(groups):
        first = lax.rem(lax.axis_index("grp") + groups - shift, groups) * half

        def body(index, total, first=first):
            return total + ref[first + index, start:, :]

        out.append(each(half, body, jnp.zeros((ref.shape[1] - start, ref.shape[2]), F32)))
    return out


def half_kernel(*refs, groups):
    got_ref = refs[0]
    pick_refs = refs[1 : 1 + groups]
    (mine_ref, near_ref, near_a_ref, near_b_ref, rhs_ref, noise_ref, basis_ref,
     part_ref, left_ref, high_ref, low_ref, far_ref, base_ref, coeff_ref, gram_ref) = refs[1 + groups :]
    rhs_rows, skel = coeff_ref.shape
    dim = part_ref.shape[1] - rhs_rows
    left = stack_left(mine_ref[0, 0:dim, :])
    left_ref[...] = left
    far_ref[...] = far_part(got_ref, groups, left, high_ref, low_ref, dim, rhs_rows)
    for index, part in enumerate(picked(got_ref, pick_refs, 0, dim, rhs_rows)):
        part_ref[index] = part
    near = near_ref[...] + near_a_ref[...] + near_b_ref[...]
    base = (noise_ref[...] - SHIFT) * rhs_ref[...] + near
    base_ref[...] = base
    basis = basis_ref[...]
    both = pair(basis)
    coeff_ref[...] = times(base, both)
    flat = basis.T
    square = raw(jnp.concatenate(split2(flat), axis=0), both)
    gram_ref[...] = (
        square[:skel, :skel] + square[:skel, skel:] + (square[skel:, :skel] + square[skel:, skel:])
    )


def first_image_kernel(*refs, groups):
    got_ref = refs[0]
    pick_refs = refs[1 : 1 + groups]
    (part_ref, left_ref, far_ref, base_ref, coeff_ref, gram_ref, rhs_ref, lift_ref, basis_ref,
     shift_ref, send_ref, top_high_ref, top_low_ref, high_ref, low_ref) = refs[1 + groups :]
    rhs_rows, skel = coeff_ref.shape
    dim = part_ref.shape[1] - rhs_rows
    parts = picked(got_ref, pick_refs, 1, dim, rhs_rows)
    parts = [part + part_ref[index] for index, part in enumerate(parts)]
    far = far_ref[...] + far_part(got_ref, groups, left_ref[...], high_ref, low_ref, dim, rhs_rows)
    left = stack_left(parts[0][0:dim])
    right = stack_right(jnp.concatenate([part[0:dim] for part in parts], axis=1))
    high, low = split2(matern3(raw(left, right)))
    top_high_ref[...] = high
    top_low_ref[...] = low
    top = times_parts_t(jnp.concatenate([part[dim:] for part in parts], axis=1), high, low)
    lift = pair(lift_ref[0])
    row = (far + times_t(top, lift)) * THIRD
    coeff = coeff_ref[...] + times(row, pair(gram_ref[...]))
    lifted = times(coeff, lift)
    rhs = rhs_ref[...]
    shift = base_ref[...] + times_t(row, pair(basis_ref[...]))
    shift_ref[...] = shift
    total = to_row(row_sum(rhs * rhs))
    along = to_row(row_sum(rhs * shift))
    rest = jnp.zeros((send_ref.shape[1] - 2 * rhs_rows - 2, skel), F32)
    fill(send_ref, jnp.concatenate([coeff, lifted, total, along, rest], axis=0))


def half_again_kernel(
    got_ref, near_ref, near_a_ref, near_b_ref, shift_ref, noise_ref, high_ref, low_ref,
    part_ref, far_ref, base_ref,
):
    rhs_rows = far_ref.shape[0]
    groups = part_ref.shape[0]
    far_ref[...] = far_again(got_ref, groups, high_ref, low_ref, rhs_rows)
    for index, part in enumerate(group_sums(got_ref, groups, rhs_rows)):
        part_ref[index] = part
    near = near_ref[...] + near_a_ref[...] + near_b_ref[...]
    base_ref[...] = noise_ref[...] * shift_ref[...] + near


def second_image_kernel(
    got_ref, part_ref, far_ref, base_ref, high_ref, low_ref, top_high_ref, top_low_ref,
    rhs_ref, shift_ref, lift_ref, basis_ref, residual_ref, image_ref, alpha_ref, send_ref,
):
    rhs_rows, skel = far_ref.shape
    groups = part_ref.shape[0]
    far = far_ref[...] + far_again(got_ref, groups, high_ref, low_ref, rhs_rows)
    parts = group_sums(got_ref, groups, rhs_rows)
    parts = [part + part_ref[index] for index, part in enumerate(parts)]
    coeff = jnp.concatenate([part[0:rhs_rows] for part in parts], axis=1)
    top = times_parts_t(coeff, top_high_ref[...], top_low_ref[...])
    sums = sum(part[rhs_rows : rhs_rows + 8] for part in parts)
    total = to_column(sums[0:1], rhs_rows)
    along = to_column(sums[1:2], rhs_rows)
    curve = along + SHIFT * total
    alpha = total / curve
    keep = along / curve
    shift = shift_ref[...]
    rhs = rhs_ref[...]
    row = (far + times_t(top, pair(lift_ref[0]))) * THIRD
    residual = keep * rhs - alpha * shift
    second = base_ref[...] + times_t(row, pair(basis_ref[...]))
    image = keep * (shift + SHIFT * rhs) - alpha * second
    residual_ref[...] = residual
    image_ref[...] = image
    lane = lax.broadcasted_iota(jnp.int32, (rhs_rows, skel), 1)
    index = lax.broadcasted_iota(jnp.int32, (rhs_rows, skel), 0)
    alpha_ref[...] = jnp.where(lane == 0, alpha, total)
    both = jnp.where(lane == index, row_sum(residual * residual), 0.0)
    both = both + jnp.where(lane == index + rhs_rows, row_sum(residual * image), 0.0)
    fill(send_ref, jnp.sum(both, axis=0, keepdims=True))


def finish_kernel(
    got_ref, alpha_ref, rhs_ref, shift_ref, residual_ref, image_ref, solution_ref, out_ref
):
    rhs_rows = rhs_ref.shape[0]
    sums = jnp.sum(got_ref[...], axis=0)
    norm_next = to_column(sums, rhs_rows)
    curve = to_column(sums, rhs_rows, rhs_rows)
    alpha = alpha_ref[:, 0:1]
    norm_now = alpha_ref[:, 1:2]
    ratio = norm_next / norm_now
    step = norm_next / (curve - ratio * norm_next / alpha)
    rhs = rhs_ref[...]
    residual = residual_ref[...]
    image = shift_ref[...] + SHIFT * rhs
    solution_ref[...] = alpha * rhs + step * (residual + ratio * rhs)
    out_ref[...] = residual - step * (image_ref[...] + ratio * image)


def spread(value, members=None):
    return lax.all_to_all(
        value, ("grp", "leaf"), 0, 0, tiled=True, axis_index_groups=members
    )


def pass_on(value, pairs, axis="leaf"):
    return lax.ppermute(value, axis, pairs)


def local(points, rhs, basis, transfer, noise, inv_scale, links, leaf_skel, group_skel):
    dim, width = points.shape
    rhs_rows = rhs.shape[0]
    skel = basis.shape[1]
    boxes = lax.axis_size("leaf")
    groups = lax.axis_size("grp")
    half = boxes // 2
    assert boxes == 2 * half
    noise = noise[None, :]
    pairs_a = [(i, i ^ 1) for i in range(boxes)]
    pairs_b = [(i, ((i + 1) ^ 1) - 1) for i in range(1, boxes - 1)]
    members = [[2 * i + c for i in range(groups * half)] for c in range(2)]
    wide = (rhs_rows, width)
    small = (rhs_rows, skel)
    step, count = box_chunks(half)
    far_shape = ((count, skel, step * skel), BF16)
    top_shape = ((skel, groups * skel), BF16)

    rows = -(-(dim + 2 * rhs_rows) // 8) * 8
    rows_next = -(-(2 * rhs_rows + 2) // 8) * 8
    room = 8 + (2 * groups * half * rows * skel * 4 + 4 * half * skel * skel * 4) // MIB
    inputs = [points, rhs, basis, transfer, noise, inv_scale, links, leaf_skel]
    scratch = [pltpu.VMEM(value.shape, value.dtype) for value in inputs]
    for index in (5, 6):
        scratch[index] = pltpu.SMEM(inputs[index].shape, inputs[index].dtype)
    beside, send, weight = call(
        prepare_kernel,
        [((dim + rhs_rows, width), F32), ((groups * half, rows, skel), F32), ((8, skel), F32)],
        inputs, space=pltpu.HBM, scratch=scratch + [pltpu.SemaphoreType.DMA((8,))],
        limit=60,
    )
    got = spread(send, members)
    beside_a = pass_on(beside, pairs_a)
    beside_b = pass_on(beside, pairs_b)
    picks = [group_skel] + [
        pass_on(
            group_skel, [(i, (i + s) % groups) for i in range(groups)],
            "grp",
        )
        for s in range(1, groups)
    ]

    def near_part(other, vec, kind):
        return call(
            functools.partial(near_kernel, kind=kind), [(wide, F32)],
            [weight, beside, other, vec], limit=16, flops=4 * 10**9,
        )[0]

    near = near_part(beside, beside, 0)
    near_a = near_part(beside_a, beside_a, 1)
    near_b = near_part(beside_b, beside_b, 2)
    peer = pass_on(got, pairs_a)
    part, left, high, low, far, base, coeff, gram = call(
        functools.partial(half_kernel, groups=groups),
        [((groups, dim + rhs_rows, skel), F32), ((skel, skel), BF16), far_shape, far_shape,
         (small, F32), (wide, F32), (small, F32), ((skel, skel), F32)],
        [got, *picks, send, near, near_a, near_b, rhs, noise, basis],
        limit=room, flops=10**9,
    )
    shift, send, top_high, top_low, peer_high, peer_low = call(
        functools.partial(first_image_kernel, groups=groups),
        [(wide, F32), ((groups * half, rows_next, skel), F32), top_shape, top_shape,
         far_shape, far_shape],
        [peer, *picks, part, left, far, base, coeff, gram, rhs, transfer, basis],
        limit=room,
    )
    got = spread(send, members)
    shift_a = pass_on(shift, pairs_a)
    shift_b = pass_on(shift, pairs_b)
    near = near_part(beside, shift, 0)
    near_a = near_part(beside_a, shift_a, 1)
    near_b = near_part(beside_b, shift_b, 2)
    peer = pass_on(got, pairs_a)
    part, far, base = call(
        half_again_kernel,
        [((groups, rows_next - rhs_rows, skel), F32), (small, F32), (wide, F32)],
        [got, near, near_a, near_b, shift, noise, high, low],
        limit=room, flops=10**9,
    )
    residual, image, alpha, send = call(
        second_image_kernel,
        [(wide, F32), (wide, F32), (small, F32), ((boxes * groups, 1, skel), F32)],
        [peer, part, far, base, peer_high, peer_low, top_high, top_low, rhs, shift, transfer, basis],
        limit=room,
    )
    got = spread(send)
    return tuple(
        call(
            finish_kernel, [(wide, F32), (wide, F32)],
            [got, alpha, rhs, shift, residual, image],
        )
    )


def solution(mesh):
    return jax.shard_map(
        local,
        mesh=mesh,
        in_specs=(
            P(None, ("grp", "leaf")),
            P(None, ("grp", "leaf")),
            P(("grp", "leaf"), None),
            P(("grp", "leaf"), None, None),
            P(("grp", "leaf")),
            P(),
            P(("grp", "leaf"), None),
            P(("grp", "leaf"), None),
            P("grp", None),
        ),
        out_specs=(P(None, ("grp", "leaf")), P(None, ("grp", "leaf"))),
        check_vma=False,
    )
```

```python
import functools
import math

import jax
import jax.numpy as jnp
from jax import lax
from jax.experimental import pallas as pl
from jax.experimental.pallas import tpu as pltpu
from jax.sharding import PartitionSpec as P


F32 = jnp.float32
BF16 = jnp.bfloat16
LOG2E = math.log2(math.e)
UNIT = math.sqrt(5.0)
THIRD = 1.0 / 3.0
MIB = 1 << 20
SHIFT = 3.0


def raw(first, second):
    return lax.dot_general(
        first, second, (((1,), (0,)), ((), ())), preferred_element_type=F32
    )


def raw_t(first, second):
    return lax.dot_general(
        first, second, (((1,), (1,)), ((), ())), preferred_element_type=F32
    )


def split3(value):
    high = value.astype(BF16).astype(F32)
    rest = value - high
    middle = rest.astype(BF16).astype(F32)
    return high, middle, (rest - middle).astype(BF16).astype(F32)


def split2(value):
    high = value.astype(BF16)
    return high, (value - high.astype(F32)).astype(BF16)


def triple(value):
    return jnp.concatenate(split3(value), axis=0).astype(BF16)


def fold(value):
    rows = value.shape[0] // 3
    return value[0:rows] + value[rows : 2 * rows] + value[2 * rows :]


def pair(value):
    return jnp.concatenate(split2(value), axis=1)


def times(first, second):
    half = second.shape[1] // 2
    both = fold(raw(triple(first), second))
    return both[:, :half] + both[:, half:]


def times_t(first, second):
    parts = triple(first)
    return fold(raw_t(jnp.concatenate([parts, parts], axis=1), second))


def times_parts_t(first, high, low):
    parts = triple(first)
    return fold(raw_t(parts, high) + raw_t(parts, low))


def norm_rows(scaled):
    high, middle, low = split3(jnp.sum(scaled * scaled, axis=0, keepdims=True))
    one = jnp.ones_like(high)
    zero = jnp.zeros((2,) + high.shape[1:], F32)
    return high, middle, low, one, zero


def stack_left(scaled):
    high, middle, low = split3(scaled)
    n_high, n_middle, n_low, one, zero = norm_rows(scaled)
    norms = jnp.concatenate([n_high, n_middle, n_low, one, one, one, zero], axis=0)
    rows = [high, high, middle, middle, high, low, norms]
    used = 6 * scaled.shape[0] + 8
    rows.append(jnp.zeros((128 - used, scaled.shape[1]), F32))
    return jnp.concatenate(rows, axis=0).T.astype(BF16)


def stack_right(scaled):
    high, middle, low = split3(-2.0 * scaled)
    n_high, n_middle, n_low, one, zero = norm_rows(scaled)
    norms = jnp.concatenate([one, one, one, n_high, n_middle, n_low, zero], axis=0)
    rows = [high, middle, high, middle, low, high, norms]
    used = 6 * scaled.shape[0] + 8
    rows.append(jnp.zeros((128 - used, scaled.shape[1]), F32))
    return jnp.concatenate(rows, axis=0).astype(BF16)


def matern3(square):
    square = jnp.maximum(square, 1e-30)
    root = square * lax.rsqrt(square)
    base = root + 1.5
    return (base * base + 0.75) * jnp.exp2(root * (-LOG2E))


def to_row(column):
    shape = (column.shape[0], 128)
    mask = lax.broadcasted_iota(jnp.int32, shape, 0) == lax.broadcasted_iota(jnp.int32, shape, 1)
    return jnp.sum(jnp.where(mask, column, 0.0), axis=0, keepdims=True)


def to_column(row, rows, start=0):
    shape = (rows, 128)
    lane = lax.broadcasted_iota(jnp.int32, shape, 1)
    mask = lane == lax.broadcasted_iota(jnp.int32, shape, 0) + start
    return jnp.sum(jnp.where(mask, row, 0.0), axis=1, keepdims=True)


def row_sum(value):
    return jnp.sum(value, axis=1, keepdims=True)


def each(count, body, init):
    if count <= 16:
        for index in range(count):
            init = body(index, init)
        return init
    return lax.fori_loop(0, count, body, init)


def fill(ref, block):
    def put(index, carry):
        ref[index] = block
        return carry

    each(ref.shape[0], put, 0)


def call(kernel, outs, ins, space=pltpu.VMEM, scratch=(), limit=8, flops=1_000_000):
    return pl.pallas_call(
        kernel,
        out_shape=[jax.ShapeDtypeStruct(s, d) for s, d in outs],
        in_specs=[pl.BlockSpec(memory_space=space) for _ in ins],
        out_specs=[pl.BlockSpec(memory_space=pltpu.VMEM) for _ in outs],
        scratch_shapes=list(scratch),
        compiler_params=pltpu.CompilerParams(vmem_limit_bytes=limit * MIB),
        cost_estimate=pl.CostEstimate(flops=flops, bytes_accessed=1 << 20, transcendentals=0),
    )(*ins)


def prepare_kernel(
    points_hbm, rhs_hbm, basis_hbm, lift_hbm, scale_hbm, links_hbm, skel_hbm,
    beside_ref, send_ref, weight_ref,
    points_ref, rhs_ref, basis_ref, lift_ref, scale_ref, links_ref, skel_ref, sems,
):
    sources = (points_hbm, scale_hbm, links_hbm, rhs_hbm, skel_hbm, basis_hbm, lift_hbm)
    targets = (points_ref, scale_ref, links_ref, rhs_ref, skel_ref, basis_ref, lift_ref)
    copies = [
        pltpu.make_async_copy(source, target, sems.at[index])
        for index, (source, target) in enumerate(zip(sources, targets))
    ]
    for copy in copies:
        copy.start()
    for copy in copies[:4]:
        copy.wait()
    dim, width = points_ref.shape
    rhs_rows = rhs_ref.shape[0]
    rows, skel = send_ref.shape[1:]
    sub = lax.broadcasted_iota(jnp.int32, (dim, 1), 0)
    scale = jnp.zeros((dim, 1), F32)
    for d in range(dim):
        scale = jnp.where(sub == d, scale_ref[d], scale)
    scaled = points_ref[...] * scale * UNIT
    rhs = rhs_ref[...]
    beside_ref[0:dim, :] = scaled
    beside_ref[dim:, :] = rhs
    lower, upper = links_ref[0, 0].astype(F32), links_ref[0, 1].astype(F32)
    odd = lax.rem(lax.axis_index("leaf"), 2).astype(F32)
    own = 1.0 + lower + upper
    first = odd * lower + (1.0 - odd) * upper
    second = odd * upper + (1.0 - odd) * lower
    sub = lax.broadcasted_iota(jnp.int32, weight_ref.shape, 0)
    weight = jnp.where(sub == 0, own, jnp.where(sub == 1, first, second))
    weight_ref[...] = weight * THIRD
    copies[4].wait()
    pick = lax.broadcasted_iota(jnp.int32, (width, skel), 0) == skel_ref[...]
    chosen = fold(raw(triple(scaled), jnp.where(pick, 1.0, 0.0).astype(BF16)))
    copies[5].wait()
    coeff = times(rhs, pair(basis_ref[...]))
    copies[6].wait()
    lifted = times(coeff, pair(lift_ref[0]))
    parts = [chosen, coeff, lifted]
    if rows > dim + 2 * rhs_rows:
        parts.append(jnp.zeros((rows - dim - 2 * rhs_rows, skel), F32))
    fill(send_ref, jnp.concatenate(parts, axis=0))


def near_kernel(weight_ref, own_ref, other_ref, vec_ref, out_ref, *, kind):
    rhs_rows, width = out_ref.shape
    dim = own_ref.shape[0] - rhs_rows
    start = vec_ref.shape[0] - rhs_rows
    block = min(256, width)
    left = stack_left(other_ref[0:dim, :])
    right = stack_right(own_ref[0:dim, :])
    vec = triple(vec_ref[start:, :])
    weight = weight_ref[kind : kind + 1, 0:1]
    for c in range(width // block):
        cols = slice(c * block, (c + 1) * block)
        total = jnp.zeros((3 * rhs_rows, block), F32)
        for i in range(width // block):
            rows = slice(i * block, (i + 1) * block)
            high, low = split2(matern3(raw(left[rows], right[:, cols])))
            total = total + raw(vec[:, rows], high) + raw(vec[:, rows], low)
        out_ref[:, cols] = fold(total) * weight


def box_chunks(boxes):
    step = min(boxes, 16)
    while boxes % step:
        step -= 1
    return step, boxes // step


def picked(ref, pick_refs, swapped, dim, rhs_rows):
    skel = ref.shape[2]
    groups = len(pick_refs)
    half = ref.shape[0] // groups
    parity = lax.rem(lax.axis_index("leaf") + swapped, 2)
    out = []
    for shift, pick_ref in enumerate(pick_refs):
        first = lax.rem(lax.axis_index("grp") + groups - shift, groups) * half

        def body(index, carry, first=first, pick_ref=pick_ref):
            chosen, summed = carry
            block = ref[first + index]
            place = lax.broadcasted_iota(jnp.int32, (skel, skel), 0)
            pick = place + (2 * index + parity) * skel == pick_ref[...]
            pick = jnp.where(pick, 1.0, 0.0).astype(BF16)
            chosen = chosen + raw(triple(block[0:dim]), pick)
            return chosen, summed + block[dim + rhs_rows : dim + 2 * rhs_rows]

        zero = (jnp.zeros((3 * dim, skel), F32), jnp.zeros((rhs_rows, skel), F32))
        chosen, summed = each(half, body, zero)
        out.append(jnp.concatenate([fold(chosen), summed], axis=0))
    return out


def far_part(ref, groups, left, high_ref, low_ref, dim, rhs_rows):
    skel = ref.shape[2]
    half = ref.shape[0] // groups
    first = lax.axis_index("grp") * half
    step, count = box_chunks(half)

    def body(index, total):
        blocks = [ref[first + index * step + j] for j in range(step)]
        right = stack_right(jnp.concatenate([block[0:dim] for block in blocks], axis=1))
        coeff = jnp.concatenate([block[dim : dim + rhs_rows] for block in blocks], axis=1)
        high, low = split2(matern3(raw(left, right)))
        high_ref[index] = high
        low_ref[index] = low
        return total + times_parts_t(coeff, high, low)

    return each(count, body, jnp.zeros((rhs_rows, skel), F32))


def far_again(ref, groups, high_ref, low_ref, rhs_rows):
    skel = ref.shape[2]
    half = ref.shape[0] // groups
    first = lax.axis_index("grp") * half
    step, count = box_chunks(half)

    def body(index, total):
        blocks = [ref[first + index * step + j, 0:rhs_rows, :] for j in range(step)]
        coeff = jnp.concatenate(blocks, axis=1)
        return total + times_parts_t(coeff, high_ref[index], low_ref[index])

    return each(count, body, jnp.zeros((rhs_rows, skel), F32))


def group_sums(ref, groups, start):
    half = ref.shape[0] // groups
    out = []
    for shift in range(groups):
        first = lax.rem(lax.axis_index("grp") + groups - shift, groups) * half

        def body(index, total, first=first):
            return total + ref[first + index, start:, :]

        out.append(each(half, body, jnp.zeros((ref.shape[1] - start, ref.shape[2]), F32)))
    return out


def half_kernel(*refs, groups):
    got_ref = refs[0]
    pick_refs = refs[1 : 1 + groups]
    (mine_ref, near_ref, near_a_ref, rhs_ref, noise_ref, basis_ref,
     part_ref, left_ref, high_ref, low_ref, far_ref, base_ref, coeff_ref, gram_ref) = refs[1 + groups :]
    rhs_rows, skel = coeff_ref.shape
    dim = part_ref.shape[1] - rhs_rows
    left = stack_left(mine_ref[0, 0:dim, :])
    left_ref[...] = left
    far_ref[...] = far_part(got_ref, groups, left, high_ref, low_ref, dim, rhs_rows)
    for index, part in enumerate(picked(got_ref, pick_refs, 0, dim, rhs_rows)):
        part_ref[index] = part
    base = (noise_ref[...] - SHIFT) * rhs_ref[...] + (near_ref[...] + near_a_ref[...])
    base_ref[...] = base
    basis = basis_ref[...]
    both = pair(basis)
    coeff_ref[...] = times(base, both)
    flat = basis.T
    square = raw(jnp.concatenate(split2(flat), axis=0), both)
    gram_ref[...] = (
        square[:skel, :skel] + square[:skel, skel:] + (square[skel:, :skel] + square[skel:, skel:])
    )


def first_image_kernel(*refs, groups):
    got_ref = refs[0]
    pick_refs = refs[1 : 1 + groups]
    (near_b_ref, part_ref, left_ref, far_ref, base_ref, coeff_ref, gram_ref, rhs_ref, lift_ref, basis_ref,
     shift_ref, send_ref, top_high_ref, top_low_ref, high_ref, low_ref) = refs[1 + groups :]
    rhs_rows, skel = coeff_ref.shape
    dim = part_ref.shape[1] - rhs_rows
    parts = picked(got_ref, pick_refs, 1, dim, rhs_rows)
    parts = [part + part_ref[index] for index, part in enumerate(parts)]
    far = far_ref[...] + far_part(got_ref, groups, left_ref[...], high_ref, low_ref, dim, rhs_rows)
    left = stack_left(parts[0][0:dim])
    right = stack_right(jnp.concatenate([part[0:dim] for part in parts], axis=1))
    high, low = split2(matern3(raw(left, right)))
    top_high_ref[...] = high
    top_low_ref[...] = low
    top = times_parts_t(jnp.concatenate([part[dim:] for part in parts], axis=1), high, low)
    lift = pair(lift_ref[0])
    row = (far + times_t(top, lift)) * THIRD
    near = near_b_ref[...]
    basis = pair(basis_ref[...])
    coeff = (coeff_ref[...] + times(near, basis)) + times(row, pair(gram_ref[...]))
    lifted = times(coeff, lift)
    rhs = rhs_ref[...]
    shift = (base_ref[...] + near) + times_t(row, basis)
    shift_ref[...] = shift
    total = to_row(row_sum(rhs * rhs))
    along = to_row(row_sum(rhs * shift))
    rest = jnp.zeros((send_ref.shape[1] - 2 * rhs_rows - 2, skel), F32)
    fill(send_ref, jnp.concatenate([coeff, lifted, total, along, rest], axis=0))


def half_again_kernel(
    got_ref, near_ref, near_a_ref, shift_ref, noise_ref, high_ref, low_ref,
    part_ref, far_ref, base_ref,
):
    rhs_rows = far_ref.shape[0]
    groups = part_ref.shape[0]
    far_ref[...] = far_again(got_ref, groups, high_ref, low_ref, rhs_rows)
    for index, part in enumerate(group_sums(got_ref, groups, rhs_rows)):
        part_ref[index] = part
    base_ref[...] = noise_ref[...] * shift_ref[...] + (near_ref[...] + near_a_ref[...])


def second_image_kernel(
    got_ref, near_b_ref, part_ref, far_ref, base_ref, high_ref, low_ref, top_high_ref, top_low_ref,
    rhs_ref, shift_ref, lift_ref, basis_ref, residual_ref, image_ref, alpha_ref, send_ref,
):
    rhs_rows, skel = far_ref.shape
    groups = part_ref.shape[0]
    far = far_ref[...] + far_again(got_ref, groups, high_ref, low_ref, rhs_rows)
    parts = group_sums(got_ref, groups, rhs_rows)
    parts = [part + part_ref[index] for index, part in enumerate(parts)]
    coeff = jnp.concatenate([part[0:rhs_rows] for part in parts], axis=1)
    top = times_parts_t(coeff, top_high_ref[...], top_low_ref[...])
    sums = sum(part[rhs_rows : rhs_rows + 8] for part in parts)
    total = to_column(sums[0:1], rhs_rows)
    along = to_column(sums[1:2], rhs_rows)
    curve = along + SHIFT * total
    alpha = total / curve
    keep = along / curve
    shift = shift_ref[...]
    rhs = rhs_ref[...]
    row = (far + times_t(top, pair(lift_ref[0]))) * THIRD
    residual = keep * rhs - alpha * shift
    second = (base_ref[...] + near_b_ref[...]) + times_t(row, pair(basis_ref[...]))
    image = keep * (shift + SHIFT * rhs) - alpha * second
    residual_ref[...] = residual
    image_ref[...] = image
    lane = lax.broadcasted_iota(jnp.int32, (rhs_rows, skel), 1)
    index = lax.broadcasted_iota(jnp.int32, (rhs_rows, skel), 0)
    alpha_ref[...] = jnp.where(lane == 0, alpha, total)
    both = jnp.where(lane == index, row_sum(residual * residual), 0.0)
    both = both + jnp.where(lane == index + rhs_rows, row_sum(residual * image), 0.0)
    fill(send_ref, jnp.sum(both, axis=0, keepdims=True))


def finish_kernel(
    got_ref, alpha_ref, rhs_ref, shift_ref, residual_ref, image_ref, solution_ref, out_ref
):
    rhs_rows = rhs_ref.shape[0]
    sums = jnp.sum(got_ref[...], axis=0)
    norm_next = to_column(sums, rhs_rows)
    curve = to_column(sums, rhs_rows, rhs_rows)
    alpha = alpha_ref[:, 0:1]
    norm_now = alpha_ref[:, 1:2]
    ratio = norm_next / norm_now
    step = norm_next / (curve - ratio * norm_next / alpha)
    rhs = rhs_ref[...]
    residual = residual_ref[...]
    image = shift_ref[...] + SHIFT * rhs
    solution_ref[...] = alpha * rhs + step * (residual + ratio * rhs)
    out_ref[...] = residual - step * (image_ref[...] + ratio * image)


def spread(value, members=None):
    return lax.all_to_all(
        value, ("grp", "leaf"), 0, 0, tiled=True, axis_index_groups=members
    )


def pass_on(value, pairs, axis="leaf"):
    return lax.ppermute(value, axis, pairs)


def local(points, rhs, basis, transfer, noise, inv_scale, links, leaf_skel, group_skel):
    dim, width = points.shape
    rhs_rows = rhs.shape[0]
    skel = basis.shape[1]
    boxes = lax.axis_size("leaf")
    groups = lax.axis_size("grp")
    half = boxes // 2
    assert boxes == 2 * half
    noise = noise[None, :]
    pairs_a = [(i, i ^ 1) for i in range(boxes)]
    pairs_b = [(i, ((i + 1) ^ 1) - 1) for i in range(1, boxes - 1)]
    members = [[2 * i + c for i in range(groups * half)] for c in range(2)]
    wide = (rhs_rows, width)
    small = (rhs_rows, skel)
    step, count = box_chunks(half)
    far_shape = ((count, skel, step * skel), BF16)
    top_shape = ((skel, groups * skel), BF16)

    rows = -(-(dim + 2 * rhs_rows) // 8) * 8
    rows_next = -(-(2 * rhs_rows + 2) // 8) * 8
    room = 8 + (2 * groups * half * rows * skel * 4 + 4 * half * skel * skel * 4) // MIB
    inputs = [points, rhs, basis, transfer, inv_scale, links, leaf_skel]
    scratch = [pltpu.VMEM(value.shape, value.dtype) for value in inputs]
    for index in (4, 5):
        scratch[index] = pltpu.SMEM(inputs[index].shape, inputs[index].dtype)
    beside, send, weight = call(
        prepare_kernel,
        [((dim + rhs_rows, width), F32), ((groups * half, rows, skel), F32), ((8, skel), F32)],
        inputs, space=pltpu.HBM, scratch=scratch + [pltpu.SemaphoreType.DMA((7,))],
        limit=60,
    )
    got = spread(send, members)
    beside_a = pass_on(beside, pairs_a)
    beside_b = pass_on(beside, pairs_b)
    picks = [group_skel] + [
        pass_on(
            group_skel, [(i, (i + s) % groups) for i in range(groups)],
            "grp",
        )
        for s in range(1, groups)
    ]

    def near_part(other, vec, kind):
        return call(
            functools.partial(near_kernel, kind=kind), [(wide, F32)],
            [weight, beside, other, vec], limit=16, flops=4 * 10**9,
        )[0]

    near = near_part(beside, beside, 0)
    near_a = near_part(beside_a, beside_a, 1)
    near_b = near_part(beside_b, beside_b, 2)
    peer = pass_on(got, pairs_a)
    part, left, high, low, far, base, coeff, gram = call(
        functools.partial(half_kernel, groups=groups),
        [((groups, dim + rhs_rows, skel), F32), ((skel, skel), BF16), far_shape, far_shape,
         (small, F32), (wide, F32), (small, F32), ((skel, skel), F32)],
        [got, *picks, send, near, near_a, rhs, noise, basis],
        limit=room, flops=10**9,
    )
    shift, send, top_high, top_low, peer_high, peer_low = call(
        functools.partial(first_image_kernel, groups=groups),
        [(wide, F32), ((groups * half, rows_next, skel), F32), top_shape, top_shape,
         far_shape, far_shape],
        [peer, *picks, near_b, part, left, far, base, coeff, gram, rhs, transfer, basis],
        limit=room,
    )
    got = spread(send, members)
    shift_a = pass_on(shift, pairs_a)
    shift_b = pass_on(shift, pairs_b)
    near = near_part(beside, shift, 0)
    near_a = near_part(beside_a, shift_a, 1)
    near_b = near_part(beside_b, shift_b, 2)
    peer = pass_on(got, pairs_a)
    part, far, base = call(
        half_again_kernel,
        [((groups, rows_next - rhs_rows, skel), F32), (small, F32), (wide, F32)],
        [got, near, near_a, shift, noise, high, low],
        limit=room, flops=10**9,
    )
    residual, image, alpha, send = call(
        second_image_kernel,
        [(wide, F32), (wide, F32), (small, F32), ((boxes * groups, 1, skel), F32)],
        [peer, near_b, part, far, base, peer_high, peer_low, top_high, top_low,
         rhs, shift, transfer, basis],
        limit=room,
    )
    got = spread(send)
    return tuple(
        call(
            finish_kernel, [(wide, F32), (wide, F32)],
            [got, alpha, rhs, shift, residual, image],
        )
    )


def solution(mesh):
    return jax.shard_map(
        local,
        mesh=mesh,
        in_specs=(
            P(None, ("grp", "leaf")),
            P(None, ("grp", "leaf")),
            P(("grp", "leaf"), None),
            P(("grp", "leaf"), None, None),
            P(("grp", "leaf")),
            P(),
            P(("grp", "leaf"), None),
            P(("grp", "leaf"), None),
            P("grp", None),
        ),
        out_specs=(P(None, ("grp", "leaf")), P(None, ("grp", "leaf"))),
        check_vma=False,
    )
```

```python
import functools
import math

import jax
import jax.numpy as jnp
from jax import lax
from jax.experimental import pallas as pl
from jax.experimental.pallas import tpu as pltpu
from jax.sharding import PartitionSpec as P


F32 = jnp.float32
BF16 = jnp.bfloat16
LOG2E = math.log2(math.e)
UNIT = math.sqrt(5.0) / 3.0
MIB = 1 << 20
SHIFT = 3.0


def raw(first, second):
    return lax.dot_general(
        first, second, (((1,), (0,)), ((), ())), preferred_element_type=F32
    )


def raw_t(first, second):
    return lax.dot_general(
        first, second, (((1,), (1,)), ((), ())), preferred_element_type=F32
    )


def split3(value):
    high = value.astype(BF16).astype(F32)
    rest = value - high
    middle = rest.astype(BF16).astype(F32)
    return high, middle, (rest - middle).astype(BF16).astype(F32)


def split2(value):
    high = value.astype(BF16)
    return high, (value - high.astype(F32)).astype(BF16)


def triple(value):
    return jnp.concatenate(split3(value), axis=0).astype(BF16)


def fold(value):
    rows = value.shape[0] // 3
    return value[0:rows] + value[rows : 2 * rows] + value[2 * rows :]


def pair(value):
    return jnp.concatenate(split2(value), axis=1)


def times(first, second):
    half = second.shape[1] // 2
    both = fold(raw(triple(first), second))
    return both[:, :half] + both[:, half:]


def times_t(first, second):
    parts = triple(first)
    return fold(raw_t(jnp.concatenate([parts, parts], axis=1), second))


def times_parts_t(first, high, low):
    parts = triple(first)
    return fold(raw_t(parts, high) + raw_t(parts, low))


def norm_rows(scaled):
    high, middle, low = split3(jnp.sum(scaled * scaled, axis=0, keepdims=True))
    one = jnp.ones_like(high)
    zero = jnp.zeros((2,) + high.shape[1:], F32)
    return high, middle, low, one, zero


def stack_left(scaled):
    high, middle, low = split3(scaled)
    n_high, n_middle, n_low, one, zero = norm_rows(scaled)
    norms = jnp.concatenate([n_high, n_middle, n_low, one, one, one, zero], axis=0)
    rows = [high, high, middle, middle, high, low, norms]
    used = 6 * scaled.shape[0] + 8
    rows.append(jnp.zeros((128 - used, scaled.shape[1]), F32))
    return jnp.concatenate(rows, axis=0).T.astype(BF16)


def stack_right(scaled):
    high, middle, low = split3(-2.0 * scaled)
    n_high, n_middle, n_low, one, zero = norm_rows(scaled)
    norms = jnp.concatenate([one, one, one, n_high, n_middle, n_low, zero], axis=0)
    rows = [high, middle, high, middle, low, high, norms]
    used = 6 * scaled.shape[0] + 8
    rows.append(jnp.zeros((128 - used, scaled.shape[1]), F32))
    return jnp.concatenate(rows, axis=0).astype(BF16)


def matern(square):
    square = jnp.maximum(square, 1e-30)
    root = square * lax.rsqrt(square)
    return ((square + root) + 1.0 / 3.0) * jnp.exp2(root * (-3.0 * LOG2E))


def to_row(column):
    shape = (column.shape[0], 128)
    mask = lax.broadcasted_iota(jnp.int32, shape, 0) == lax.broadcasted_iota(jnp.int32, shape, 1)
    return jnp.sum(jnp.where(mask, column, 0.0), axis=0, keepdims=True)


def to_column(row, rows, start=0):
    shape = (rows, 128)
    lane = lax.broadcasted_iota(jnp.int32, shape, 1)
    mask = lane == lax.broadcasted_iota(jnp.int32, shape, 0) + start
    return jnp.sum(jnp.where(mask, row, 0.0), axis=1, keepdims=True)


def row_sum(value):
    return jnp.sum(value, axis=1, keepdims=True)


def each(count, body, init):
    if count <= 16:
        for index in range(count):
            init = body(index, init)
        return init
    return lax.fori_loop(0, count, body, init)


def fill(ref, block, first=0, count=None):
    def put(index, carry):
        ref[first + index] = block
        return carry

    each(ref.shape[0] if count is None else count, put, 0)


def call(kernel, outs, ins, space=pltpu.VMEM, scratch=(), limit=8, flops=1_000_000):
    return pl.pallas_call(
        kernel,
        out_shape=[jax.ShapeDtypeStruct(s, d) for s, d in outs],
        in_specs=[pl.BlockSpec(memory_space=space) for _ in ins],
        out_specs=[pl.BlockSpec(memory_space=pltpu.VMEM) for _ in outs],
        scratch_shapes=list(scratch),
        compiler_params=pltpu.CompilerParams(vmem_limit_bytes=limit * MIB),
        cost_estimate=pl.CostEstimate(flops=flops, bytes_accessed=1 << 20, transcendentals=0),
    )(*ins)


def prepare_kernel(
    points_hbm, rhs_hbm, basis_hbm, lift_hbm, scale_hbm, links_hbm, skel_hbm, pick_hbm,
    beside_ref, send_ref, weight_ref, mine_ref,
    points_ref, rhs_ref, basis_ref, lift_ref, scale_ref, links_ref, skel_ref, pick_ref, sems,
    *, groups,
):
    sources = (points_hbm, scale_hbm, links_hbm, rhs_hbm, skel_hbm, basis_hbm, lift_hbm, pick_hbm)
    targets = (points_ref, scale_ref, links_ref, rhs_ref, skel_ref, basis_ref, lift_ref, pick_ref)
    copies = [
        pltpu.make_async_copy(source, target, sems.at[index])
        for index, (source, target) in enumerate(zip(sources, targets))
    ]
    for copy in copies:
        copy.start()
    for copy in copies[:4]:
        copy.wait()
    dim, width = points_ref.shape
    rhs_rows = rhs_ref.shape[0]
    rows, skel = send_ref.shape[1:]
    sub = lax.broadcasted_iota(jnp.int32, (dim, 1), 0)
    scale = jnp.zeros((dim, 1), F32)
    for d in range(dim):
        scale = jnp.where(sub == d, scale_ref[d], scale)
    scaled = points_ref[...] * scale * UNIT
    rhs = rhs_ref[...]
    beside_ref[0:dim, :] = scaled
    beside_ref[dim:, :] = rhs
    lower, upper = links_ref[0, 0].astype(F32), links_ref[0, 1].astype(F32)
    odd = lax.rem(lax.axis_index("leaf"), 2).astype(F32)
    own = 1.0 + lower + upper
    first = odd * lower + (1.0 - odd) * upper
    second = odd * upper + (1.0 - odd) * lower
    sub = lax.broadcasted_iota(jnp.int32, weight_ref.shape, 0)
    weight = jnp.where(sub == 0, own, jnp.where(sub == 1, first, second))
    weight_ref[...] = weight * 3.0
    copies[4].wait()
    pick = lax.broadcasted_iota(jnp.int32, (width, skel), 0) == skel_ref[...]
    chosen = fold(raw(triple(scaled), jnp.where(pick, 1.0, 0.0).astype(BF16)))
    copies[5].wait()
    coeff = times(rhs, pair(basis_ref[...]))
    copies[6].wait()
    lifted = times(coeff, pair(lift_ref[0]))
    copies[7].wait()
    index = jnp.concatenate([pick_ref[...].astype(F32), jnp.zeros((rhs_rows - 1, skel), F32)], axis=0)
    mine_ref[...] = jnp.concatenate([chosen, coeff, index], axis=0)
    rest = [lifted]
    if rows > dim + 2 * rhs_rows:
        rest.append(jnp.zeros((rows - dim - 2 * rhs_rows, skel), F32))
    half = send_ref.shape[0] // groups
    for shift in range(groups):
        first = lax.rem(lax.axis_index("grp") + shift, groups) * half
        middle = index if shift else coeff
        fill(send_ref, jnp.concatenate([chosen, middle, *rest], axis=0), first, half)


def self_kernel(weight_ref, own_ref, vec_ref, out_ref, high_ref, low_ref):
    rhs_rows, width = out_ref.shape
    dim = own_ref.shape[0] - rhs_rows
    start = vec_ref.shape[0] - rhs_rows
    block = min(256, width)
    left = stack_left(own_ref[0:dim, :])
    right = stack_right(own_ref[0:dim, :])
    vec = triple(vec_ref[start:, :])
    weight = weight_ref[0:1, 0:1]
    count = width // block
    for c in range(count):
        cols = slice(c * block, (c + 1) * block)
        for i in range(c + 1):
            rows = slice(i * block, (i + 1) * block)
            high, low = split2(matern(raw(left[rows], right[:, cols])))
            high_ref[rows, cols] = high
            low_ref[rows, cols] = low
    for c in range(count):
        cols = slice(c * block, (c + 1) * block)
        above = slice(0, (c + 1) * block)
        total = raw(vec[:, above], high_ref[above, cols]) + raw(vec[:, above], low_ref[above, cols])
        if c + 1 < count:
            rest = slice((c + 1) * block, width)
            total = total + raw_t(vec[:, rest], high_ref[cols, rest])
            total = total + raw_t(vec[:, rest], low_ref[cols, rest])
        out_ref[:, cols] = fold(total) * weight


def near_kernel(weight_ref, own_ref, other_ref, vec_ref, out_ref, *, kind):
    rhs_rows, width = out_ref.shape
    dim = own_ref.shape[0] - rhs_rows
    start = vec_ref.shape[0] - rhs_rows
    block = min(256, width)
    left = stack_left(other_ref[0:dim, :])
    right = stack_right(own_ref[0:dim, :])
    vec = triple(vec_ref[start:, :])
    weight = weight_ref[kind : kind + 1, 0:1]
    for c in range(width // block):
        cols = slice(c * block, (c + 1) * block)
        total = jnp.zeros((3 * rhs_rows, block), F32)
        for i in range(width // block):
            rows = slice(i * block, (i + 1) * block)
            high, low = split2(matern(raw(left[rows], right[:, cols])))
            total = total + raw(vec[:, rows], high) + raw(vec[:, rows], low)
        out_ref[:, cols] = fold(total) * weight


def box_chunks(boxes):
    step = min(boxes, 16)
    while boxes % step:
        step -= 1
    return step, boxes // step


def picked(ref, mine_ref, groups, swapped, dim, rhs_rows):
    skel = ref.shape[2]
    half = ref.shape[0] // groups
    parity = lax.rem(lax.axis_index("leaf") + swapped, 2)
    out = []
    for shift in range(groups):
        first = lax.rem(lax.axis_index("grp") + groups - shift, groups) * half
        if shift:
            wanted = ref[first, dim : dim + 1, :]
        else:
            wanted = mine_ref[dim + rhs_rows : dim + rhs_rows + 1, :]
        wanted = wanted.astype(jnp.int32)

        def body(index, carry, first=first, wanted=wanted):
            chosen, summed = carry
            block = ref[first + index]
            place = lax.broadcasted_iota(jnp.int32, (skel, skel), 0)
            pick = place + (2 * index + parity) * skel == wanted
            pick = jnp.where(pick, 1.0, 0.0).astype(BF16)
            chosen = chosen + raw(triple(block[0:dim]), pick)
            return chosen, summed + block[dim + rhs_rows : dim + 2 * rhs_rows]

        zero = (jnp.zeros((3 * dim, skel), F32), jnp.zeros((rhs_rows, skel), F32))
        chosen, summed = each(half, body, zero)
        out.append(jnp.concatenate([fold(chosen), summed], axis=0))
    return out


def far_part(ref, groups, left, high_ref, low_ref, dim, rhs_rows):
    skel = ref.shape[2]
    half = ref.shape[0] // groups
    first = lax.axis_index("grp") * half
    step, count = box_chunks(half)

    def body(index, total):
        blocks = [ref[first + index * step + j] for j in range(step)]
        right = stack_right(jnp.concatenate([block[0:dim] for block in blocks], axis=1))
        coeff = jnp.concatenate([block[dim : dim + rhs_rows] for block in blocks], axis=1)
        high, low = split2(matern(raw(left, right)))
        high_ref[index] = high
        low_ref[index] = low
        return total + times_parts_t(coeff, high, low)

    return each(count, body, jnp.zeros((rhs_rows, skel), F32))


def far_again(ref, groups, high_ref, low_ref, rhs_rows):
    skel = ref.shape[2]
    half = ref.shape[0] // groups
    first = lax.axis_index("grp") * half
    step, count = box_chunks(half)

    def body(index, total):
        blocks = [ref[first + index * step + j, 0:rhs_rows, :] for j in range(step)]
        coeff = jnp.concatenate(blocks, axis=1)
        return total + times_parts_t(coeff, high_ref[index], low_ref[index])

    return each(count, body, jnp.zeros((rhs_rows, skel), F32))


def group_sums(ref, groups, start):
    half = ref.shape[0] // groups
    out = []
    for shift in range(groups):
        first = lax.rem(lax.axis_index("grp") + groups - shift, groups) * half

        def body(index, total, first=first):
            return total + ref[first + index, start:, :]

        out.append(each(half, body, jnp.zeros((ref.shape[1] - start, ref.shape[2]), F32)))
    return out


def base_kernel(
    mine_ref, near_ref, near_a_ref, rhs_ref, noise_ref, basis_ref,
    base_ref, coeff_ref, gram_ref, copy_ref,
):
    skel = basis_ref.shape[1]
    copy_ref[...] = mine_ref[...]
    base = (noise_ref[...] - SHIFT) * rhs_ref[...] + (near_ref[...] + near_a_ref[...])
    base_ref[...] = base
    basis = basis_ref[...]
    both = pair(basis)
    coeff_ref[...] = times(base, both)
    square = raw(jnp.concatenate(split2(basis.T), axis=0), both)
    gram_ref[...] = (
        square[:skel, :skel] + square[:skel, skel:] + (square[skel:, :skel] + square[skel:, skel:])
    )


def half_kernel(
    got_ref, mine_ref, part_ref, left_ref, high_ref, low_ref, far_ref, *, groups
):
    rhs_rows = far_ref.shape[0]
    dim = part_ref.shape[1] - rhs_rows
    left = stack_left(mine_ref[0:dim, :])
    left_ref[...] = left
    far_ref[...] = far_part(got_ref, groups, left, high_ref, low_ref, dim, rhs_rows)
    for index, part in enumerate(picked(got_ref, mine_ref, groups, 0, dim, rhs_rows)):
        part_ref[index] = part


def first_image_kernel(*refs, groups):
    (got_ref, near_b_ref, part_ref, left_ref, far_ref, base_ref, coeff_ref, gram_ref, mine_ref, rhs_ref, lift_ref, basis_ref,
     shift_ref, send_ref, top_high_ref, top_low_ref, high_ref, low_ref) = refs
    rhs_rows, skel = coeff_ref.shape
    dim = part_ref.shape[1] - rhs_rows
    parts = picked(got_ref, mine_ref, groups, 1, dim, rhs_rows)
    parts = [part + part_ref[index] for index, part in enumerate(parts)]
    far = far_ref[...] + far_part(got_ref, groups, left_ref[...], high_ref, low_ref, dim, rhs_rows)
    left = stack_left(parts[0][0:dim])
    right = stack_right(jnp.concatenate([part[0:dim] for part in parts], axis=1))
    high, low = split2(matern(raw(left, right)))
    top_high_ref[...] = high
    top_low_ref[...] = low
    top = times_parts_t(jnp.concatenate([part[dim:] for part in parts], axis=1), high, low)
    lift = pair(lift_ref[0])
    row = (far + times_t(top, lift)) * 3.0
    near = near_b_ref[...]
    basis = pair(basis_ref[...])
    coeff = (coeff_ref[...] + times(near, basis)) + times(row, pair(gram_ref[...]))
    lifted = times(coeff, lift)
    rhs = rhs_ref[...]
    base = base_ref[...] + near
    total = to_row(row_sum(rhs * rhs))
    along = to_row(row_sum(rhs * base) + row_sum(mine_ref[dim : dim + rhs_rows, :] * row))
    rest = jnp.zeros((send_ref.shape[1] - 2 * rhs_rows - 2, skel), F32)
    fill(send_ref, jnp.concatenate([coeff, lifted, total, along, rest], axis=0))
    shift_ref[...] = base + times_t(row, basis)


def half_again_kernel(
    got_ref, near_ref, near_a_ref, shift_ref, noise_ref, high_ref, low_ref,
    part_ref, far_ref, base_ref,
):
    rhs_rows = far_ref.shape[0]
    groups = part_ref.shape[0]
    far_ref[...] = far_again(got_ref, groups, high_ref, low_ref, rhs_rows)
    for index, part in enumerate(group_sums(got_ref, groups, rhs_rows)):
        part_ref[index] = part
    base_ref[...] = noise_ref[...] * shift_ref[...] + (near_ref[...] + near_a_ref[...])


def second_image_kernel(
    got_ref, near_b_ref, part_ref, far_ref, base_ref, high_ref, low_ref, top_high_ref, top_low_ref,
    rhs_ref, shift_ref, lift_ref, basis_ref, residual_ref, image_ref, alpha_ref, send_ref,
):
    rhs_rows, skel = far_ref.shape
    groups = part_ref.shape[0]
    far = far_ref[...] + far_again(got_ref, groups, high_ref, low_ref, rhs_rows)
    parts = group_sums(got_ref, groups, rhs_rows)
    parts = [part + part_ref[index] for index, part in enumerate(parts)]
    coeff = jnp.concatenate([part[0:rhs_rows] for part in parts], axis=1)
    top = times_parts_t(coeff, top_high_ref[...], top_low_ref[...])
    sums = sum(part[rhs_rows : rhs_rows + 8] for part in parts)
    total = to_column(sums[0:1], rhs_rows)
    along = to_column(sums[1:2], rhs_rows)
    curve = along + SHIFT * total
    alpha = total / curve
    keep = along / curve
    shift = shift_ref[...]
    rhs = rhs_ref[...]
    row = (far + times_t(top, pair(lift_ref[0]))) * 3.0
    residual = keep * rhs - alpha * shift
    second = (base_ref[...] + near_b_ref[...]) + times_t(row, pair(basis_ref[...]))
    image = keep * (shift + SHIFT * rhs) - alpha * second
    residual_ref[...] = residual
    image_ref[...] = image
    lane = lax.broadcasted_iota(jnp.int32, (rhs_rows, skel), 1)
    index = lax.broadcasted_iota(jnp.int32, (rhs_rows, skel), 0)
    alpha_ref[...] = jnp.where(lane == 0, alpha, total)
    both = jnp.where(lane == index, row_sum(residual * residual), 0.0)
    both = both + jnp.where(lane == index + rhs_rows, row_sum(residual * image), 0.0)
    fill(send_ref, jnp.sum(both, axis=0, keepdims=True))


def finish_kernel(
    got_ref, alpha_ref, rhs_ref, shift_ref, residual_ref, image_ref, solution_ref, out_ref
):
    rhs_rows = rhs_ref.shape[0]
    sums = jnp.sum(got_ref[...], axis=0)
    norm_next = to_column(sums, rhs_rows)
    curve = to_column(sums, rhs_rows, rhs_rows)
    alpha = alpha_ref[:, 0:1]
    norm_now = alpha_ref[:, 1:2]
    ratio = norm_next / norm_now
    step = norm_next / (curve - ratio * norm_next / alpha)
    rhs = rhs_ref[...]
    residual = residual_ref[...]
    image = shift_ref[...] + SHIFT * rhs
    solution_ref[...] = alpha * rhs + step * (residual + ratio * rhs)
    out_ref[...] = residual - step * (image_ref[...] + ratio * image)


def spread(value, members=None):
    return lax.all_to_all(
        value, ("grp", "leaf"), 0, 0, tiled=True, axis_index_groups=members
    )


def pass_on(value, pairs, axis="leaf"):
    return lax.ppermute(value, axis, pairs)


def local(points, rhs, basis, transfer, noise, inv_scale, links, leaf_skel, group_skel):
    dim, width = points.shape
    rhs_rows = rhs.shape[0]
    skel = basis.shape[1]
    boxes = lax.axis_size("leaf")
    groups = lax.axis_size("grp")
    half = boxes // 2
    assert boxes == 2 * half
    noise = noise[None, :]
    pairs_a = [(i, i ^ 1) for i in range(boxes)]
    pairs_b = [(i, ((i + 1) ^ 1) - 1) for i in range(1, boxes - 1)]
    members = [[2 * i + c for i in range(groups * half)] for c in range(2)]
    wide = (rhs_rows, width)
    small = (rhs_rows, skel)
    step, count = box_chunks(half)
    far_shape = ((count, skel, step * skel), BF16)
    top_shape = ((skel, groups * skel), BF16)

    rows = -(-(dim + 2 * rhs_rows) // 8) * 8
    rows_next = -(-(2 * rhs_rows + 2) // 8) * 8
    room = 8 + (2 * groups * half * rows * skel * 4 + 4 * half * skel * skel * 4) // MIB
    mine_shape = (dim + 2 * rhs_rows, skel)
    inputs = [points, rhs, basis, transfer, inv_scale, links, leaf_skel, group_skel]
    scratch = [pltpu.VMEM(value.shape, value.dtype) for value in inputs]
    for index in (4, 5):
        scratch[index] = pltpu.SMEM(inputs[index].shape, inputs[index].dtype)
    beside, send, weight, mine = call(
        functools.partial(prepare_kernel, groups=groups),
        [((dim + rhs_rows, width), F32), ((groups * half, rows, skel), F32), ((8, skel), F32),
         (mine_shape, F32)],
        inputs, space=pltpu.HBM, scratch=scratch + [pltpu.SemaphoreType.DMA((8,))],
        limit=60,
    )
    got = spread(send, members)
    beside_a = pass_on(beside, pairs_a)
    beside_b = pass_on(beside, pairs_b)

    def near_part(other, vec, kind):
        return call(
            functools.partial(near_kernel, kind=kind), [(wide, F32)],
            [weight, beside, other, vec], limit=16, flops=4 * 10**9,
        )[0]

    def self_part(vec):
        return call(
            self_kernel, [(wide, F32)], [weight, beside, vec],
            scratch=[pltpu.VMEM((width, width), BF16)] * 2, limit=16, flops=4 * 10**9,
        )[0]

    near = self_part(beside)
    near_a = near_part(beside_a, beside_a, 1)
    near_b = near_part(beside_b, beside_b, 2)
    peer = pass_on(got, pairs_a)
    base, coeff, gram, mine = call(
        base_kernel, [(wide, F32), (small, F32), ((skel, skel), F32), (mine_shape, F32)],
        [mine, near, near_a, rhs, noise, basis], flops=10**9,
    )
    part, left, high, low, far = call(
        functools.partial(half_kernel, groups=groups),
        [((groups, dim + rhs_rows, skel), F32), ((skel, skel), BF16), far_shape, far_shape,
         (small, F32)],
        [got, mine], limit=room, flops=10**9,
    )
    shift, send, top_high, top_low, peer_high, peer_low = call(
        functools.partial(first_image_kernel, groups=groups),
        [(wide, F32), ((groups * half, rows_next, skel), F32), top_shape, top_shape,
         far_shape, far_shape],
        [peer, near_b, part, left, far, base, coeff, gram, mine, rhs, transfer, basis],
        limit=room,
    )
    got = spread(send, members)
    shift_a = pass_on(shift, pairs_a)
    shift_b = pass_on(shift, pairs_b)
    near = self_part(shift)
    near_a = near_part(beside_a, shift_a, 1)
    near_b = near_part(beside_b, shift_b, 2)
    peer = pass_on(got, pairs_a)
    part, far, base = call(
        half_again_kernel,
        [((groups, rows_next - rhs_rows, skel), F32), (small, F32), (wide, F32)],
        [got, near, near_a, shift, noise, high, low],
        limit=room, flops=10**9,
    )
    residual, image, alpha, send = call(
        second_image_kernel,
        [(wide, F32), (wide, F32), (small, F32), ((boxes * groups, 1, skel), F32)],
        [peer, near_b, part, far, base, peer_high, peer_low, top_high, top_low,
         rhs, shift, transfer, basis],
        limit=room,
    )
    got = spread(send)
    return tuple(
        call(
            finish_kernel, [(wide, F32), (wide, F32)],
            [got, alpha, rhs, shift, residual, image],
        )
    )


def solution(mesh):
    return jax.shard_map(
        local,
        mesh=mesh,
        in_specs=(
            P(None, ("grp", "leaf")),
            P(None, ("grp", "leaf")),
            P(("grp", "leaf"), None),
            P(("grp", "leaf"), None, None),
            P(("grp", "leaf")),
            P(),
            P(("grp", "leaf"), None),
            P(("grp", "leaf"), None),
            P("grp", None),
        ),
        out_specs=(P(None, ("grp", "leaf")), P(None, ("grp", "leaf"))),
        check_vma=False,
    )
```

```python
import functools
import math

import jax
import jax.numpy as jnp
from jax import lax
from jax.experimental import pallas as pl
from jax.experimental.pallas import tpu as pltpu
from jax.sharding import PartitionSpec as P


F32 = jnp.float32
BF16 = jnp.bfloat16
LOG2E = math.log2(math.e)
UNIT = math.sqrt(5.0) / 3.0
MIB = 1 << 20
SHIFT = 3.0


def raw(first, second):
    return lax.dot_general(
        first, second, (((1,), (0,)), ((), ())), preferred_element_type=F32
    )


def raw_t(first, second):
    return lax.dot_general(
        first, second, (((1,), (1,)), ((), ())), preferred_element_type=F32
    )


def split3(value):
    high = value.astype(BF16).astype(F32)
    rest = value - high
    middle = rest.astype(BF16).astype(F32)
    return high, middle, (rest - middle).astype(BF16).astype(F32)


def split2(value):
    high = value.astype(BF16)
    return high, (value - high.astype(F32)).astype(BF16)


def triple(value):
    return jnp.concatenate(split3(value), axis=0).astype(BF16)


def fold(value):
    rows = value.shape[0] // 3
    return value[0:rows] + value[rows : 2 * rows] + value[2 * rows :]


def pair(value):
    return jnp.concatenate(split2(value), axis=1)


def times(first, second):
    half = second.shape[1] // 2
    both = fold(raw(triple(first), second))
    return both[:, :half] + both[:, half:]


def times_t(first, second):
    parts = triple(first)
    return fold(raw_t(jnp.concatenate([parts, parts], axis=1), second))


def times_parts_t(first, high, low):
    parts = triple(first)
    return fold(raw_t(parts, high) + raw_t(parts, low))


def norm_rows(scaled):
    high, middle, low = split3(jnp.sum(scaled * scaled, axis=0, keepdims=True))
    one = jnp.ones_like(high)
    zero = jnp.zeros((2,) + high.shape[1:], F32)
    return high, middle, low, one, zero


def stack_left(scaled):
    high, middle, low = split3(scaled)
    n_high, n_middle, n_low, one, zero = norm_rows(scaled)
    norms = jnp.concatenate([n_high, n_middle, n_low, one, one, one, zero], axis=0)
    rows = [high, high, middle, middle, high, low, norms]
    used = 6 * scaled.shape[0] + 8
    rows.append(jnp.zeros((128 - used, scaled.shape[1]), F32))
    return jnp.concatenate(rows, axis=0).T.astype(BF16)


def stack_right(scaled):
    high, middle, low = split3(-2.0 * scaled)
    n_high, n_middle, n_low, one, zero = norm_rows(scaled)
    norms = jnp.concatenate([one, one, one, n_high, n_middle, n_low, zero], axis=0)
    rows = [high, middle, high, middle, low, high, norms]
    used = 6 * scaled.shape[0] + 8
    rows.append(jnp.zeros((128 - used, scaled.shape[1]), F32))
    return jnp.concatenate(rows, axis=0).astype(BF16)


def matern(square):
    square = jnp.maximum(square, 1e-30)
    root = square * lax.rsqrt(square)
    return ((square + root) + 1.0 / 3.0) * jnp.exp2(root * (-3.0 * LOG2E))


def to_row(column):
    shape = (column.shape[0], 128)
    mask = lax.broadcasted_iota(jnp.int32, shape, 0) == lax.broadcasted_iota(jnp.int32, shape, 1)
    return jnp.sum(jnp.where(mask, column, 0.0), axis=0, keepdims=True)


def to_column(row, rows, start=0):
    shape = (rows, 128)
    lane = lax.broadcasted_iota(jnp.int32, shape, 1)
    mask = lane == lax.broadcasted_iota(jnp.int32, shape, 0) + start
    return jnp.sum(jnp.where(mask, row, 0.0), axis=1, keepdims=True)


def row_sum(value):
    return jnp.sum(value, axis=1, keepdims=True)


def each(count, body, init):
    if count <= 16:
        for index in range(count):
            init = body(index, init)
        return init
    return lax.fori_loop(0, count, body, init)


def fill(ref, block, first=0, count=None):
    def put(index, carry):
        ref[first + index] = block
        return carry

    each(ref.shape[0] if count is None else count, put, 0)


def call(kernel, outs, ins, space=pltpu.VMEM, scratch=(), limit=8, flops=1_000_000):
    return pl.pallas_call(
        kernel,
        out_shape=[jax.ShapeDtypeStruct(s, d) for s, d in outs],
        in_specs=[pl.BlockSpec(memory_space=space) for _ in ins],
        out_specs=[pl.BlockSpec(memory_space=pltpu.VMEM) for _ in outs],
        scratch_shapes=list(scratch),
        compiler_params=pltpu.CompilerParams(vmem_limit_bytes=limit * MIB),
        cost_estimate=pl.CostEstimate(flops=flops, bytes_accessed=1 << 20, transcendentals=0),
    )(*ins)


def prepare_kernel(
    points_hbm, rhs_hbm, basis_hbm, lift_hbm, scale_hbm, links_hbm, skel_hbm, pick_hbm,
    beside_ref, send_ref, weight_ref, mine_ref,
    points_ref, rhs_ref, basis_ref, lift_ref, scale_ref, links_ref, skel_ref, pick_ref, sems,
    *, groups,
):
    sources = (points_hbm, scale_hbm, links_hbm, rhs_hbm, skel_hbm, basis_hbm, lift_hbm, pick_hbm)
    targets = (points_ref, scale_ref, links_ref, rhs_ref, skel_ref, basis_ref, lift_ref, pick_ref)
    copies = [
        pltpu.make_async_copy(source, target, sems.at[index])
        for index, (source, target) in enumerate(zip(sources, targets))
    ]
    for copy in copies:
        copy.start()
    for copy in copies[:4]:
        copy.wait()
    dim, width = points_ref.shape
    rhs_rows = rhs_ref.shape[0]
    rows, skel = send_ref.shape[1:]
    sub = lax.broadcasted_iota(jnp.int32, (dim, 1), 0)
    scale = jnp.zeros((dim, 1), F32)
    for d in range(dim):
        scale = jnp.where(sub == d, scale_ref[d], scale)
    scaled = points_ref[...] * scale * UNIT
    rhs = rhs_ref[...]
    beside_ref[0:dim, :] = scaled
    beside_ref[dim:, :] = rhs
    lower, upper = links_ref[0, 0].astype(F32), links_ref[0, 1].astype(F32)
    odd = lax.rem(lax.axis_index("leaf"), 2).astype(F32)
    own = 1.0 + lower + upper
    first = odd * lower + (1.0 - odd) * upper
    second = odd * upper + (1.0 - odd) * lower
    sub = lax.broadcasted_iota(jnp.int32, weight_ref.shape, 0)
    weight = jnp.where(sub == 0, own, jnp.where(sub == 1, first, second))
    weight_ref[...] = weight * 3.0
    copies[4].wait()
    pick = lax.broadcasted_iota(jnp.int32, (width, skel), 0) == skel_ref[...]
    chosen = fold(raw(triple(scaled), jnp.where(pick, 1.0, 0.0).astype(BF16)))
    copies[5].wait()
    coeff = times(rhs, pair(basis_ref[...]))
    copies[6].wait()
    lifted = times(coeff, pair(lift_ref[0]))
    copies[7].wait()
    index = jnp.concatenate([pick_ref[...].astype(F32), jnp.zeros((rhs_rows - 1, skel), F32)], axis=0)
    mine_ref[...] = jnp.concatenate([chosen, coeff, index], axis=0)
    rest = [lifted]
    if rows > dim + 2 * rhs_rows:
        rest.append(jnp.zeros((rows - dim - 2 * rhs_rows, skel), F32))
    half = send_ref.shape[0] // groups
    for shift in range(groups):
        first = lax.rem(lax.axis_index("grp") + shift, groups) * half
        middle = index if shift else coeff
        fill(send_ref, jnp.concatenate([chosen, middle, *rest], axis=0), first, half)


def self_kernel(weight_ref, own_ref, vec_ref, out_ref, high_ref, low_ref):
    rhs_rows, width = out_ref.shape
    dim = own_ref.shape[0] - rhs_rows
    start = vec_ref.shape[0] - rhs_rows
    block = min(256, width)
    left = stack_left(own_ref[0:dim, :])
    right = stack_right(own_ref[0:dim, :])
    vec = triple(vec_ref[start:, :])
    weight = weight_ref[0:1, 0:1]
    count = width // block
    for c in range(count):
        cols = slice(c * block, (c + 1) * block)
        for i in range(c + 1):
            rows = slice(i * block, (i + 1) * block)
            high, low = split2(matern(raw(left[rows], right[:, cols])))
            high_ref[rows, cols] = high
            low_ref[rows, cols] = low
    for c in range(count):
        cols = slice(c * block, (c + 1) * block)
        above = slice(0, (c + 1) * block)
        total = raw(vec[:, above], high_ref[above, cols]) + raw(vec[:, above], low_ref[above, cols])
        if c + 1 < count:
            rest = slice((c + 1) * block, width)
            total = total + raw_t(vec[:, rest], high_ref[cols, rest])
            total = total + raw_t(vec[:, rest], low_ref[cols, rest])
        out_ref[:, cols] = fold(total) * weight


def near_kernel(weight_ref, own_ref, other_ref, vec_ref, out_ref, *, kind):
    rhs_rows, width = out_ref.shape
    dim = own_ref.shape[0] - rhs_rows
    start = vec_ref.shape[0] - rhs_rows
    block = min(256, width)
    left = stack_left(other_ref[0:dim, :])
    right = stack_right(own_ref[0:dim, :])
    vec = triple(vec_ref[start:, :])
    weight = weight_ref[kind : kind + 1, 0:1]
    for c in range(width // block):
        cols = slice(c * block, (c + 1) * block)
        total = jnp.zeros((3 * rhs_rows, block), F32)
        for i in range(width // block):
            rows = slice(i * block, (i + 1) * block)
            high, low = split2(matern(raw(left[rows], right[:, cols])))
            total = total + raw(vec[:, rows], high) + raw(vec[:, rows], low)
        out_ref[:, cols] = fold(total) * weight


def box_chunks(boxes):
    step = min(boxes, 16)
    while boxes % step:
        step -= 1
    return step, boxes // step


def picked(ref, mine_ref, groups, swapped, dim, rhs_rows):
    skel = ref.shape[2]
    half = ref.shape[0] // groups
    parity = lax.rem(lax.axis_index("leaf") + swapped, 2)
    out = []
    for shift in range(groups):
        first = lax.rem(lax.axis_index("grp") + groups - shift, groups) * half
        if shift:
            wanted = ref[first, dim : dim + 1, :]
        else:
            wanted = mine_ref[dim + rhs_rows : dim + rhs_rows + 1, :]
        wanted = wanted.astype(jnp.int32)

        def body(index, carry, first=first, wanted=wanted):
            chosen, summed = carry
            block = ref[first + index]
            place = lax.broadcasted_iota(jnp.int32, (skel, skel), 0)
            pick = place + (2 * index + parity) * skel == wanted
            pick = jnp.where(pick, 1.0, 0.0).astype(BF16)
            chosen = chosen + raw(triple(block[0:dim]), pick)
            return chosen, summed + block[dim + rhs_rows : dim + 2 * rhs_rows]

        zero = (jnp.zeros((3 * dim, skel), F32), jnp.zeros((rhs_rows, skel), F32))
        chosen, summed = each(half, body, zero)
        out.append(jnp.concatenate([fold(chosen), summed], axis=0))
    return out


def far_part(ref, groups, left, high_ref, low_ref, dim, rhs_rows):
    skel = ref.shape[2]
    half = ref.shape[0] // groups
    first = lax.axis_index("grp") * half
    step, count = box_chunks(half)

    def body(index, total):
        blocks = [ref[first + index * step + j] for j in range(step)]
        right = stack_right(jnp.concatenate([block[0:dim] for block in blocks], axis=1))
        coeff = jnp.concatenate([block[dim : dim + rhs_rows] for block in blocks], axis=1)
        high, low = split2(matern(raw(left, right)))
        high_ref[index] = high
        low_ref[index] = low
        return total + times_parts_t(coeff, high, low)

    return each(count, body, jnp.zeros((rhs_rows, skel), F32))


def far_again(ref, groups, high_ref, low_ref, rhs_rows):
    skel = ref.shape[2]
    half = ref.shape[0] // groups
    first = lax.axis_index("grp") * half
    step, count = box_chunks(half)

    def body(index, total):
        blocks = [ref[first + index * step + j, 0:rhs_rows, :] for j in range(step)]
        coeff = jnp.concatenate(blocks, axis=1)
        return total + times_parts_t(coeff, high_ref[index], low_ref[index])

    return each(count, body, jnp.zeros((rhs_rows, skel), F32))


def group_sums(ref, groups, start):
    half = ref.shape[0] // groups
    out = []
    for shift in range(groups):
        first = lax.rem(lax.axis_index("grp") + groups - shift, groups) * half

        def body(index, total, first=first):
            return total + ref[first + index, start:, :]

        out.append(each(half, body, jnp.zeros((ref.shape[1] - start, ref.shape[2]), F32)))
    return out


def base_kernel(
    mine_ref, near_ref, near_a_ref, rhs_ref, noise_ref, basis_ref,
    base_ref, coeff_ref, gram_ref, copy_ref,
):
    skel = basis_ref.shape[1]
    copy_ref[...] = mine_ref[...]
    base = (noise_ref[...] - SHIFT) * rhs_ref[...] + (near_ref[...] + near_a_ref[...])
    base_ref[...] = base
    basis = basis_ref[...]
    both = pair(basis)
    coeff_ref[...] = times(base, both)
    square = raw(jnp.concatenate(split2(basis.T), axis=0), both)
    gram_ref[...] = (
        square[:skel, :skel] + square[:skel, skel:] + (square[skel:, :skel] + square[skel:, skel:])
    )


def half_kernel(
    got_ref, mine_ref, part_ref, left_ref, high_ref, low_ref, far_ref, *, groups
):
    rhs_rows = far_ref.shape[0]
    dim = part_ref.shape[1] - rhs_rows
    left = stack_left(mine_ref[0:dim, :])
    left_ref[...] = left
    far_ref[...] = far_part(got_ref, groups, left, high_ref, low_ref, dim, rhs_rows)
    for index, part in enumerate(picked(got_ref, mine_ref, groups, 0, dim, rhs_rows)):
        part_ref[index] = part


def first_image_kernel(*refs, groups):
    (got_ref, near_b_ref, part_ref, left_ref, far_ref, base_ref, coeff_ref, gram_ref, mine_ref, rhs_ref, lift_ref, basis_ref,
     shift_ref, send_ref, top_high_ref, top_low_ref, high_ref, low_ref) = refs
    rhs_rows, skel = coeff_ref.shape
    dim = part_ref.shape[1] - rhs_rows
    parts = picked(got_ref, mine_ref, groups, 1, dim, rhs_rows)
    parts = [part + part_ref[index] for index, part in enumerate(parts)]
    far = far_ref[...] + far_part(got_ref, groups, left_ref[...], high_ref, low_ref, dim, rhs_rows)
    left = stack_left(parts[0][0:dim])
    right = stack_right(jnp.concatenate([part[0:dim] for part in parts], axis=1))
    high, low = split2(matern(raw(left, right)))
    top_high_ref[...] = high
    top_low_ref[...] = low
    top = times_parts_t(jnp.concatenate([part[dim:] for part in parts], axis=1), high, low)
    lift = pair(lift_ref[0])
    row = (far + times_t(top, lift)) * 3.0
    near = near_b_ref[...]
    basis = pair(basis_ref[...])
    coeff = (coeff_ref[...] + times(near, basis)) + times(row, pair(gram_ref[...]))
    lifted = times(coeff, lift)
    rhs = rhs_ref[...]
    base = base_ref[...] + near
    total = to_row(row_sum(rhs * rhs))
    along = to_row(row_sum(rhs * base) + row_sum(mine_ref[dim : dim + rhs_rows, :] * row))
    rest = jnp.zeros((send_ref.shape[1] - 2 * rhs_rows - 2, skel), F32)
    fill(send_ref, jnp.concatenate([coeff, lifted, total, along, rest], axis=0))
    shift_ref[...] = base + times_t(row, basis)


def half_again_kernel(
    got_ref, near_ref, near_a_ref, shift_ref, noise_ref, high_ref, low_ref,
    part_ref, far_ref, base_ref,
):
    rhs_rows = far_ref.shape[0]
    groups = part_ref.shape[0]
    far_ref[...] = far_again(got_ref, groups, high_ref, low_ref, rhs_rows)
    for index, part in enumerate(group_sums(got_ref, groups, rhs_rows)):
        part_ref[index] = part
    base_ref[...] = noise_ref[...] * shift_ref[...] + (near_ref[...] + near_a_ref[...])


def lift_kernel(lift_ref, high_ref, low_ref, out_high_ref, out_low_ref):
    parts = triple(lift_ref[0])
    both = fold(raw(parts, high_ref[...]) + raw(parts, low_ref[...]))
    out_high_ref[...], out_low_ref[...] = split2(both)


def second_image_kernel(
    got_ref, near_b_ref, part_ref, far_ref, base_ref, high_ref, low_ref, top_high_ref, top_low_ref,
    rhs_ref, shift_ref, basis_ref, residual_ref, image_ref, alpha_ref, send_ref,
):
    rhs_rows, skel = far_ref.shape
    groups = part_ref.shape[0]
    far = far_ref[...] + far_again(got_ref, groups, high_ref, low_ref, rhs_rows)
    parts = group_sums(got_ref, groups, rhs_rows)
    parts = [part + part_ref[index] for index, part in enumerate(parts)]
    coeff = jnp.concatenate([part[0:rhs_rows] for part in parts], axis=1)
    top = times_parts_t(coeff, top_high_ref[...], top_low_ref[...])
    sums = sum(part[rhs_rows : rhs_rows + 8] for part in parts)
    total = to_column(sums[0:1], rhs_rows)
    along = to_column(sums[1:2], rhs_rows)
    curve = along + SHIFT * total
    alpha = total / curve
    keep = along / curve
    shift = shift_ref[...]
    rhs = rhs_ref[...]
    row = (far + top) * 3.0
    residual = keep * rhs - alpha * shift
    second = (base_ref[...] + near_b_ref[...]) + times_t(row, pair(basis_ref[...]))
    image = keep * (shift + SHIFT * rhs) - alpha * second
    residual_ref[...] = residual
    image_ref[...] = image
    lane = lax.broadcasted_iota(jnp.int32, (rhs_rows, skel), 1)
    index = lax.broadcasted_iota(jnp.int32, (rhs_rows, skel), 0)
    alpha_ref[...] = jnp.where(lane == 0, alpha, total)
    both = jnp.where(lane == index, row_sum(residual * residual), 0.0)
    both = both + jnp.where(lane == index + rhs_rows, row_sum(residual * image), 0.0)
    fill(send_ref, jnp.sum(both, axis=0, keepdims=True))


def finish_kernel(
    got_ref, alpha_ref, rhs_ref, shift_ref, residual_ref, image_ref, solution_ref, out_ref
):
    rhs_rows = rhs_ref.shape[0]
    sums = jnp.sum(got_ref[...], axis=0)
    norm_next = to_column(sums, rhs_rows)
    curve = to_column(sums, rhs_rows, rhs_rows)
    alpha = alpha_ref[:, 0:1]
    norm_now = alpha_ref[:, 1:2]
    ratio = norm_next / norm_now
    step = norm_next / (curve - ratio * norm_next / alpha)
    rhs = rhs_ref[...]
    residual = residual_ref[...]
    image = shift_ref[...] + SHIFT * rhs
    solution_ref[...] = alpha * rhs + step * (residual + ratio * rhs)
    out_ref[...] = residual - step * (image_ref[...] + ratio * image)


def spread(value, members=None):
    return lax.all_to_all(
        value, ("grp", "leaf"), 0, 0, tiled=True, axis_index_groups=members
    )


def pass_on(value, pairs, axis="leaf"):
    return lax.ppermute(value, axis, pairs)


def local(points, rhs, basis, transfer, noise, inv_scale, links, leaf_skel, group_skel):
    dim, width = points.shape
    rhs_rows = rhs.shape[0]
    skel = basis.shape[1]
    boxes = lax.axis_size("leaf")
    groups = lax.axis_size("grp")
    half = boxes // 2
    assert boxes == 2 * half
    noise = noise[None, :]
    pairs_a = [(i, i ^ 1) for i in range(boxes)]
    pairs_b = [(i, ((i + 1) ^ 1) - 1) for i in range(1, boxes - 1)]
    members = [[2 * i + c for i in range(groups * half)] for c in range(2)]
    wide = (rhs_rows, width)
    small = (rhs_rows, skel)
    step, count = box_chunks(half)
    far_shape = ((count, skel, step * skel), BF16)
    top_shape = ((skel, groups * skel), BF16)

    rows = -(-(dim + 2 * rhs_rows) // 8) * 8
    rows_next = -(-(2 * rhs_rows + 2) // 8) * 8
    room = 8 + (2 * groups * half * rows * skel * 4 + 4 * half * skel * skel * 4) // MIB
    mine_shape = (dim + 2 * rhs_rows, skel)
    inputs = [points, rhs, basis, transfer, inv_scale, links, leaf_skel, group_skel]
    scratch = [pltpu.VMEM(value.shape, value.dtype) for value in inputs]
    for index in (4, 5):
        scratch[index] = pltpu.SMEM(inputs[index].shape, inputs[index].dtype)
    beside, send, weight, mine = call(
        functools.partial(prepare_kernel, groups=groups),
        [((dim + rhs_rows, width), F32), ((groups * half, rows, skel), F32), ((8, skel), F32),
         (mine_shape, F32)],
        inputs, space=pltpu.HBM, scratch=scratch + [pltpu.SemaphoreType.DMA((8,))],
        limit=60,
    )
    got = spread(send, members)
    beside_a = pass_on(beside, pairs_a)
    beside_b = pass_on(beside, pairs_b)

    def near_part(other, vec, kind):
        return call(
            functools.partial(near_kernel, kind=kind), [(wide, F32)],
            [weight, beside, other, vec], limit=16, flops=4 * 10**9,
        )[0]

    def self_part(vec):
        return call(
            self_kernel, [(wide, F32)], [weight, beside, vec],
            scratch=[pltpu.VMEM((width, width), BF16)] * 2, limit=16, flops=4 * 10**9,
        )[0]

    near = self_part(beside)
    near_a = near_part(beside_a, beside_a, 1)
    near_b = near_part(beside_b, beside_b, 2)
    peer = pass_on(got, pairs_a)
    base, coeff, gram, mine = call(
        base_kernel, [(wide, F32), (small, F32), ((skel, skel), F32), (mine_shape, F32)],
        [mine, near, near_a, rhs, noise, basis], flops=10**9,
    )
    part, left, high, low, far = call(
        functools.partial(half_kernel, groups=groups),
        [((groups, dim + rhs_rows, skel), F32), ((skel, skel), BF16), far_shape, far_shape,
         (small, F32)],
        [got, mine], limit=room, flops=10**9,
    )
    shift, send, top_high, top_low, peer_high, peer_low = call(
        functools.partial(first_image_kernel, groups=groups),
        [(wide, F32), ((groups * half, rows_next, skel), F32), top_shape, top_shape,
         far_shape, far_shape],
        [peer, near_b, part, left, far, base, coeff, gram, mine, rhs, transfer, basis],
        limit=room,
    )
    got = spread(send, members)
    shift_a = pass_on(shift, pairs_a)
    shift_b = pass_on(shift, pairs_b)
    near = self_part(shift)
    near_a = near_part(beside_a, shift_a, 1)
    near_b = near_part(beside_b, shift_b, 2)
    peer = pass_on(got, pairs_a)
    top_high, top_low = call(
        lift_kernel, [top_shape, top_shape], [transfer, top_high, top_low], flops=10**8,
    )
    part, far, base = call(
        half_again_kernel,
        [((groups, rows_next - rhs_rows, skel), F32), (small, F32), (wide, F32)],
        [got, near, near_a, shift, noise, high, low],
        limit=room, flops=10**9,
    )
    residual, image, alpha, send = call(
        second_image_kernel,
        [(wide, F32), (wide, F32), (small, F32), ((boxes * groups, 1, skel), F32)],
        [peer, near_b, part, far, base, peer_high, peer_low, top_high, top_low,
         rhs, shift, basis],
        limit=room,
    )
    got = spread(send)
    return tuple(
        call(
            finish_kernel, [(wide, F32), (wide, F32)],
            [got, alpha, rhs, shift, residual, image],
        )
    )


def solution(mesh):
    return jax.shard_map(
        local,
        mesh=mesh,
        in_specs=(
            P(None, ("grp", "leaf")),
            P(None, ("grp", "leaf")),
            P(("grp", "leaf"), None),
            P(("grp", "leaf"), None, None),
            P(("grp", "leaf")),
            P(),
            P(("grp", "leaf"), None),
            P(("grp", "leaf"), None),
            P("grp", None),
        ),
        out_specs=(P(None, ("grp", "leaf")), P(None, ("grp", "leaf"))),
        check_vma=False,
    )
```
